32 devices in a mesh: gx: 4 (over y, x), gy: 4 (over z), gz: 2 (over core).
Axes of the slice: x: 2, y: 2, z: 4, core: 2. Of those that a mesh axis runs over, the one named last changes fastest.
Arguments:
- rhs_coarse: bfloat16 [32, 32, 128], P('gx'), may hold values from -24 to 24
- rhs_mid: bfloat16 [64, 64, 256], P('gx', 'gy'), may hold values from -24 to 24
- rhs_fine: bfloat16 [128, 128, 512], P('gx', 'gy', 'gz'), may hold values from -24 to 24
- occupied_coarse: int32 [4, 4, 16], P('gx'), may hold values 0 or 1
- occupied_mid: int32 [8, 8, 32], P('gx', 'gy'), may hold values 0 or 1
- occupied_fine: int32 [16, 16, 64], P('gx', 'gy', 'gz'), may hold values 0 or 1
- screen_weight: float32 [3], replicated, may hold values from 0.2 to 2
Outputs:
- solution_coarse: float32 [32, 32, 128], P('gx')
- solution_mid: float32 [64, 64, 256], P('gx', 'gy')
- solution_fine: float32 [128, 128, 512], P('gx', 'gy', 'gz')
The draws below stay inside these ranges and needn't reach their ends.
All inputs are finite; a program needn't handle non-finite values. No bound on the sum of `occupied_coarse` or of `occupied_mid` or of `occupied_fine` on one device may be relied on, other than what follows from the above.
Results may differ from the reference program's by a relative error of at most 0.0003.
Values sent between devices are 32-bit elements; how exact they have to be, the bound alone decides.
A program may use at most 128 MiB of HBM per device.

```python
import math
import jax
import jax.numpy as jnp
from jax import lax

BRICK = 8
CG_ITERS = 2
NX = 128
NY = 128
NZ = 512


def place_ends(drawn, key, least, top_value):
    shape = drawn.shape
    place = [jax.random.randint(jax.random.fold_in(key, axis), (), 0, shape[axis]) for axis in range(len(shape))]
    drawn = drawn.at[tuple(place)].set(least)
    longest = shape.index(max(shape))
    place[longest] = (place[longest] + 1) % shape[longest]
    return drawn.at[tuple(place)].set(top_value)


def shard_levels(key, extent, split, smallest, top_value):
    loudness = 1.0
    for dim, parts in split:
        heights = jax.random.uniform(jax.random.fold_in(jax.random.fold_in(key, 6), dim), (parts,), jnp.float32, smallest / len(split), top_value / len(split))
        loudness = loudness * jnp.repeat(jnp.exp(heights), extent[dim] // parts).reshape((-1,) + (1,) * (len(extent) - 1 - dim))
    return loudness


def centred(own_key, extent, deviation, bound, cuts=(), kind=jnp.bfloat16):
    loudness = shard_levels(own_key, extent, cuts, -0.22, 0.18) if cuts else 1.0
    values = jax.random.normal(own_key, extent, jnp.float32) * deviation * loudness
    return jnp.minimum(jnp.maximum(values, -bound), bound).astype(kind)


def setup_inputs(seed: int = 0) -> dict:
    arg_keys = jax.random.split(jax.random.key(seed), 8)
    rhs_coarse = centred(arg_keys[0], (NX // 4, NY // 4, NZ // 4), 4.0, 24.0, ((0, 4),))
    rhs_mid = centred(arg_keys[1], (NX // 2, NY // 2, NZ // 2), 4.0, 24.0, ((0, 4), (1, 4)))
    rhs_fine = centred(arg_keys[2], (NX, NY, NZ), 4.0, 24.0, ((0, 4), (1, 4), (2, 2)))
    occupied_coarse = place_ends((jax.random.randint(arg_keys[3], (NX // (4 * BRICK), NY // (4 * BRICK), NZ // (4 * BRICK)), 0, 2) < 1).astype(jnp.int32), jax.random.fold_in(arg_keys[3], 1), 0, 1)
    occupied_mid = place_ends((jax.random.randint(arg_keys[4], (NX // (2 * BRICK), NY // (2 * BRICK), NZ // (2 * BRICK)), 0, 2) < 1).astype(jnp.int32), jax.random.fold_in(arg_keys[4], 1), 0, 1)
    occupied_fine = place_ends((jax.random.randint(arg_keys[5], (NX // BRICK, NY // BRICK, NZ // BRICK), 0, 2) < 1).astype(jnp.int32), jax.random.fold_in(arg_keys[5], 1), 0, 1)
    screen_weight = jnp.clip(jnp.exp(jax.random.uniform(arg_keys[6], (3,), jnp.float32, math.log(0.2), math.log(2.0))), 0.2, 2.0)
    return {"rhs_coarse": rhs_coarse, "rhs_mid": rhs_mid, "rhs_fine": rhs_fine, "occupied_coarse": occupied_coarse, "occupied_mid": occupied_mid, "occupied_fine": occupied_fine, "screen_weight": screen_weight}


def alternate(even_cells, odd_cells, dim_index):
    stacked = jnp.stack([even_cells, odd_cells], axis=dim_index + 1)
    new_shape = list(even_cells.shape)
    new_shape[dim_index] = new_shape[dim_index] * 2
    return stacked.reshape(new_shape)


def prolong_axis(padded, dim_index, extend):
    length = padded.shape[dim_index]
    below_cells = lax.slice_in_dim(padded, 0, length - 2, axis=dim_index)
    middle = lax.slice_in_dim(padded, 1, length - 1, axis=dim_index)
    above_cells = lax.slice_in_dim(padded, 2, length, axis=dim_index)
    refined = alternate(0.75 * middle + 0.25 * below_cells, 0.75 * middle + 0.25 * above_cells, dim_index)
    if extend:
        first_rim = 0.75 * lax.slice_in_dim(padded, 0, 1, axis=dim_index) + 0.25 * lax.slice_in_dim(padded, 1, 2, axis=dim_index)
        last_rim = 0.75 * lax.slice_in_dim(padded, length - 1, length, axis=dim_index) + 0.25 * lax.slice_in_dim(padded, length - 2, length - 1, axis=dim_index)
        refined = jnp.concatenate([first_rim, refined, last_rim], axis=dim_index)
    return refined


def prolong(coarse):
    padded = jnp.pad(coarse, 1)
    for dim_index in range(3):
        padded = prolong_axis(padded, dim_index, False)
    return padded


def screening(occupied, weight):
    brick_flags = occupied.astype(jnp.float32)
    brick_shape = occupied.shape
    spread = jnp.broadcast_to(brick_flags[:, None, :, None, :, None], (brick_shape[0], BRICK, brick_shape[1], BRICK, brick_shape[2], BRICK))
    cell_flags = spread.reshape(brick_shape[0] * BRICK, brick_shape[1] * BRICK, brick_shape[2] * BRICK)
    return weight * (0.25 + cell_flags)


def stencil(padded, screen):
    centre = padded[1:-1, 1:-1, 1:-1]
    beside = padded[2:, 1:-1, 1:-1] + padded[:-2, 1:-1, 1:-1]
    beside = beside + padded[1:-1, 2:, 1:-1] + padded[1:-1, :-2, 1:-1]
    beside = beside + padded[1:-1, 1:-1, 2:] + padded[1:-1, 1:-1, :-2]
    return (6.0 + screen) * centre - beside


def cg_solve(right_side, guess, screen):
    target = right_side.astype(jnp.float32)
    iterate = guess
    residual = target - stencil(jnp.pad(iterate, 1), screen)
    direction = residual
    norm_now = jnp.sum(residual * residual)
    for turn_index in range(CG_ITERS):
        image = stencil(jnp.pad(direction, 1), screen)
        step_size = norm_now / jnp.sum(direction * image)
        iterate = iterate + step_size * direction
        residual = residual - step_size * image
        if turn_index + 1 < CG_ITERS:
            norm_next = jnp.sum(residual * residual)
            direction = residual + (norm_next / norm_now) * direction
            norm_now = norm_next
    return iterate


def reference(rhs_coarse, rhs_mid, rhs_fine, occupied_coarse, occupied_mid, occupied_fine, screen_weight):
    start_guess = jnp.zeros(rhs_coarse.shape, jnp.float32)
    solution_coarse = cg_solve(rhs_coarse, start_guess, screening(occupied_coarse, screen_weight[0]))
    solution_mid = cg_solve(rhs_mid, prolong(solution_coarse), screening(occupied_mid, screen_weight[1]))
    solution_fine = cg_solve(rhs_fine, prolong(solution_mid), screening(occupied_fine, screen_weight[2]))
    return solution_coarse, solution_mid, solution_fine
```

```python
import functools
import math

import jax
import jax.numpy as jnp
from jax import lax
from jax.experimental import pallas as pl
from jax.experimental.pallas import tpu as pltpu
from jax.sharding import PartitionSpec as P

MESH = pl.DeviceIdType.MESH
F32 = jnp.float32
BF16 = jnp.bfloat16
PAD = 4
ROWS = 8
LANES = 128
VMEM_BYTES = 67043328


def iota(shape, dim):
    return lax.broadcasted_iota(jnp.int32, shape, dim)


def logical(index, own, extra):
    if extra == 0:
        return index
    return jnp.where(index < own + extra // 2, index, index - (own + extra))


def prolong_matrix(fine, coarse, total):
    base = lax.shift_right_arithmetic(fine, 1)
    beside = base + 2 * (fine & 1) - 1
    inside = jnp.logical_and(fine >= 0, fine < total)
    value = jnp.where(coarse == base, 0.75, jnp.where(coarse == beside, 0.25, 0.0))
    return jnp.where(inside, value, 0.0).astype(BF16)


def split(values):
    high = values.astype(BF16)
    return high, (values - high.astype(F32)).astype(BF16)


def mm(a, b):
    return jnp.dot(a, b, preferred_element_type=F32)


def fold_rows(values):
    total = values[0:ROWS]
    for row in range(ROWS, values.shape[0], ROWS):
        total = total + values[row : row + ROWS]
    out = total[:, 0:LANES]
    for lane in range(LANES, values.shape[1], LANES):
        out = out + total[:, lane : lane + LANES]
    return out


def coefficients(m0, n1, n2, n3):
    rho = n1 / m0
    spread = n2 - rho * n1
    bent = 6.0 * spread + (n3 - 2.0 * rho * n2 + rho * rho * n1)
    turn = jnp.where(bent > 0.0, jnp.maximum(spread, 0.0) / bent, 0.0)
    first = m0 / ((6.0 + rho) * m0 - jnp.maximum(spread, 0.0) * turn)
    second = -first * turn
    return first - second * rho, second


def kernel(
    dims,
    rhs_c, rhs_m, rhs_f, occ_c, occ_m, occ_f, weight_in,
    out_c, out_m, fg, fr, fw, tg, tr, tw, coef,
    in_c, in_m, in_f, io_c, io_m, io_f, weight, isem,
    cr, cw, cs, cx, ctz, ct, oc,
    mb, mg, mr, mw, ms, mx, mtz, mt, om, m_up, m_dn, m_fu, m_fd, om_l, om_r,
    fb, fs, of, zsend, edge, f_up, f_dn, f_fu, f_fd, of_l, of_r,
    ac, am, af, ss, rs, sc, rc, sm, rm, sf, rf,
):
    nx, ny, nz = dims
    ix, iy, iz = lax.axis_index("gx"), lax.axis_index("gy"), lax.axis_index("gz")
    xc, yc, zc = rhs_c.shape
    xm, ym, zm = rhs_m.shape
    xf, yf, zh = rhs_f.shape
    zf = zh * nz
    xc, xm, xf = xc // nz, xm // nz, xf // nz
    slab = ix * nz + iz
    slabs = nx * nz
    bc, bm, bf = occ_c.shape, occ_m.shape, occ_f.shape
    x_low, x_high = ix > 0, ix < nx - 1
    y_low, y_high = iy > 0, iy < ny - 1
    lower, upper = iz == 0, iz == 1
    first, last = slab == 0, slab == slabs - 1

    def both(a, b):
        return jnp.logical_and(a, b)

    def at(offset):
        return (
            lax.rem(ix + offset[0], nx), lax.rem(iy + offset[1], ny), lax.rem(iz + offset[2], nz)
        )

    for ref in (oc, om, of):
        ref[...] = jnp.zeros_like(ref)

    barrier = pltpu.get_barrier_semaphore()
    peers = [(a, b, c) for a in range(nx) for b in range(ny) for c in range(nz)][1:]
    for offset in peers:
        pl.semaphore_signal(barrier, inc=1, device_id=at(offset), device_id_type=MESH)

    loads = {}
    pairs = (
        ("c", rhs_c, in_c), ("oc", occ_c, io_c), ("w", weight_in, weight), ("f", rhs_f, in_f),
        ("m", rhs_m, in_m), ("om", occ_m, io_m), ("of", occ_f, io_f),
    )
    for k, (name, src, dst) in enumerate(pairs):
        loads[name] = pltpu.make_async_copy(src, dst, isem.at[k])
        loads[name].start()

    @pl.when(first)
    def _():
        cr[0:4] = jnp.zeros((4, yc, zc), F32)
        mb[1:4, 0:ym, :] = jnp.zeros((3, ym, zm), F32)
        fb[2:4, 0:yf, :] = jnp.zeros((2, yf, zf), F32)

    @pl.when(last)
    def _():
        cr[PAD + xc : PAD + xc + 4] = jnp.zeros((4, yc, zc), F32)
        mb[PAD + xm : PAD + xm + 3, 0:ym, :] = jnp.zeros((3, ym, zm), F32)
        fb[PAD + xf : PAD + xf + 2, 0:yf, :] = jnp.zeros((2, yf, zf), F32)

    @pl.when(jnp.logical_not(x_low))
    def _():
        for ref in (om_l, om_r, of_l, of_r):
            ref[0:1] = jnp.zeros((1,) + tuple(ref.shape[1:]), F32)

    @pl.when(jnp.logical_not(x_high))
    def _():
        for ref in (om_l, om_r, of_l, of_r):
            size = ref.shape[0]
            ref[size - 1 : size] = jnp.zeros((1,) + tuple(ref.shape[1:]), F32)

    @pl.when(jnp.logical_not(y_low))
    def _():
        for ref in (m_fu, f_fu, om_l, of_l):
            ref[...] = jnp.zeros_like(ref)

    @pl.when(jnp.logical_not(y_high))
    def _():
        for ref in (m_fd, f_fd, om_r, of_r):
            ref[...] = jnp.zeros_like(ref)

    loads["c"].wait()
    cr[pl.ds(PAD - 4 * iz, xc + 4)] = in_c[pl.ds(iz * (xc - 4), xc + 4)].astype(F32)
    loads["oc"].wait()
    oc[1 : 1 + bc[0], 0 : bc[1], 0 : bc[2]] = io_c[...].astype(F32)

    pl.semaphore_wait(barrier, len(peers))

    used = [0]

    def copy(src, dst, target, step=0, count=1):
        k = used[0]
        used[0] += count
        made = [
            pltpu.make_async_remote_copy(
                src_ref=src, dst_ref=dst, send_sem=ss.at[k], recv_sem=rs.at[k + j],
                device_id=target, device_id_type=MESH,
            )
            for j in range(count)
        ]
        if count == 1:
            return made[0]
        sender = pltpu.make_async_remote_copy(
            src_ref=src, dst_ref=dst, send_sem=ss.at[k], recv_sem=rs.at[k + step],
            device_id=target, device_id_type=MESH,
        )
        return sender, made

    def start(items):
        for c, can_send, _ in items:
            if can_send is None:
                c.start()
            elif can_send is not False:
                pl.when(can_send)(c.start)

    def arrive(items):
        for c, _, can_recv in items:
            if can_recv is None:
                c.wait_recv()
            elif can_recv is not False:
                pl.when(can_recv)(c.wait_recv)

    def left(items):
        for c, can_send, _ in items:
            if can_send is None:
                c.wait_send()
            elif can_send is not False:
                pl.when(can_send)(c.wait_send)

    above, below = {"gx": ix + 1, "gz": 0}, {"gx": ix - 1, "gz": 1}
    send_up, get_low = both(upper, x_high), both(lower, x_low)
    send_down, get_high = both(lower, x_low), both(upper, x_high)

    def slab_swap(ref, own, rows, width_low, width_high, skip_low=0, skip_high=0):
        items = []
        stop = PAD + own - skip_low
        items.append((copy(ref.at[stop - width_low : stop, 0:rows, :],
                           ref.at[PAD - skip_low - width_low : PAD - skip_low, 0:rows, :], above),
                      send_up, get_low))
        begin = PAD + skip_high
        items.append((copy(ref.at[begin : begin + width_high, 0:rows, :],
                           ref.at[begin + own : begin + own + width_high, 0:rows, :], below),
                      send_down, get_high))
        return items

    def x_flags(occ, bricks):
        return [
            (copy(occ.at[bricks], occ.at[0], {"gx": ix + 1}), x_high, x_low),
            (copy(occ.at[1], occ.at[bricks + 1], {"gx": ix - 1}), x_low, x_high),
        ]

    def y_flags(occ, occ_l, occ_r, bricks):
        items = []
        flags = pl.ds(1, bricks)
        for dst, step, can_send, can_recv in (
            (occ_l, 1, y_high, y_low), (occ_r, -1, y_low, y_high)
        ):
            items.append((copy(occ.at[flags], dst.at[flags], {"gy": iy + step}), can_send, can_recv))
            items.append((copy(occ.at[bricks], dst.at[0], {"gx": ix + 1, "gy": iy + step}),
                          both(can_send, x_high), both(can_recv, x_low)))
            items.append((copy(occ.at[1], dst.at[bricks + 1], {"gx": ix - 1, "gy": iy + step}),
                          both(can_send, x_low), both(can_recv, x_high)))
        return items

    def y_swap(ref, own, rows, width, low, high, to_up, to_down, from_low, from_high):
        span = slice(PAD - low, PAD + own + high)
        to_up[...] = ref[span, rows - width : rows, :]
        to_down[...] = ref[span, 0:width, :]
        return [
            (copy(to_up, from_low, {"gy": iy + 1}), y_high, y_low),
            (copy(to_down, from_high, {"gy": iy - 1}), y_low, y_high),
        ]

    def y_merge(ref, own, width, from_low, from_high, begin):
        count = from_low.shape[0]
        parts = [from_high[...], from_low[...]]
        if 2 * width < ROWS:
            parts.insert(1, jnp.zeros((count, ROWS - 2 * width, ref.shape[2]), F32))
        ref[begin : begin + count, own : own + ROWS, :] = jnp.concatenate(parts, axis=1)

    near = slab_swap(cr, xc, yc, 1, 2) + x_flags(oc, bc[0])
    start(near)
    far = slab_swap(cr, xc, yc, 3, 2, 1, 2)
    start(far)

    loads["f"].wait()
    own_z = pl.ds(pl.multiple_of(iz * zh, LANES), zh)
    other = 1 - iz

    def fill_fine(j, carry):
        zsend[j] = in_f[other * (xf - 2) + j].astype(F32)
        fb[PAD - 2 * iz + j, 0:yf, own_z] = in_f[iz * (xf - 2) + j].astype(F32)
        return carry

    lax.fori_loop(0, xf + 2, fill_fine, 0)
    loads["of"].wait()
    own_flags = pl.ds(pl.multiple_of(iz * LANES, LANES), LANES)
    flags = jnp.concatenate(
        [io_f[...].astype(F32), jnp.zeros((bf[0], bf[1], LANES - bf[2]), F32)], axis=2
    )
    of[1 : 1 + bf[0], 0 : bf[1], own_flags] = flags
    partner = {"gz": other}
    z_fine = [
        (copy(zsend, fb.at[pl.ds(PAD - 2 * other, xf + 2), 0:yf, own_z], partner), None, None),
        (copy(of.at[pl.ds(1, bf[0]), :, own_flags], of.at[pl.ds(1, bf[0]), :, own_flags], partner),
         None, None),
    ]
    start(z_fine)

    loads["m"].wait()
    mb[pl.ds(PAD - 3 * iz, xm + 3), 0:ym, :] = in_m[pl.ds(iz * (xm - 3), xm + 3)].astype(F32)
    loads["om"].wait()
    om[1 : 1 + bm[0], 0 : bm[1], 0 : bm[2]] = io_m[...].astype(F32)
    mid_x = slab_swap(mb, xm, ym, 3, 3)
    start(mid_x)
    mid_flags = x_flags(om, bm[0]) + y_flags(om, om_l, om_r, bm[0])
    start(mid_flags)
    edge[0:2] = in_f[0:2].astype(F32)
    edge[2] = in_f[nz * xf - 1].astype(F32)

    def row_prolong(own, extra, index, total, cols, col_own, col_extra, col_index):
        shape = (own + extra, cols)
        fine = logical(iota(shape, 0), own, extra) + own * index
        coarse = logical(iota(shape, 1), col_own, col_extra) + col_own * col_index
        return prolong_matrix(fine, coarse, total)

    def lane_prolong(cells, rows):
        shape = (rows, cells)
        return prolong_matrix(iota(shape, 1), iota(shape, 0), cells)

    def lane_bricks(cells, bricks, halves):
        shape = (halves * LANES, cells)
        brick = lax.div(iota(shape, 1), cells // (bricks * halves))
        place = brick + lax.div(brick, bricks) * (LANES - bricks)
        return (place == iota(shape, 0)).astype(BF16)

    def screens(dest, occ_parts, own, extra_rows, bricks_y, lane_matrix, level):
        count = dest.shape[0]
        side = own // bricks_y
        cols = ROWS * len(occ_parts)
        shape = (dest.shape[1], cols)
        brick = lax.div(logical(iota(shape, 0), own, extra_rows) + side, side) - 1
        place = jnp.where(
            brick < 0, ROWS + bricks_y - 1, jnp.where(brick >= bricks_y, 2 * ROWS, brick)
        )
        row_matrix = (place == iota(shape, 1)).astype(BF16)
        for x in range(count):
            flags = jnp.concatenate([part[x] for part in occ_parts], axis=0).astype(BF16)
            wide = mm(flags, lane_matrix).astype(BF16)
            dest[x] = weight[level] * (0.25 + mm(row_matrix, wide))

    def along_y(v):
        n = v.shape[0]
        return pltpu.roll(v, 1, 0), pltpu.roll(v, n - 1, 0)

    def z_up(v):
        n = v.shape[1]
        turned = pltpu.roll(v, 1, 1)
        edge_lane = iota((v.shape[0], LANES), 1) == 0
        fixed = jnp.where(edge_lane, 0.0, turned[:, 0:LANES])
        return fixed if n == LANES else jnp.concatenate([fixed, turned[:, LANES:]], axis=1)

    def z_down(v):
        n = v.shape[1]
        turned = pltpu.roll(v, n - 1, 1)
        edge_lane = iota((v.shape[0], LANES), 1) == LANES - 1
        fixed = jnp.where(edge_lane, 0.0, turned[:, n - LANES :])
        return fixed if n == LANES else jnp.concatenate([turned[:, : n - LANES], fixed], axis=1)

    loads["w"].wait()
    lanes_c = lane_bricks(zc, bc[2], 1)
    side_c = nz * xc // bc[0]
    shape_c = (yc, zc)
    row_c = iota(shape_c, 0)

    def sum_c(v, twice):
        yu, yd = along_y(v)
        total = jnp.where(row_c < yc - 1, yd, 0.0) + z_down(v)
        if twice:
            total = total + jnp.where(row_c > 0, yu, 0.0) + z_up(v)
        return total

    def brick_of(own, side):
        return lambda p: lax.div(own * iz + p + (side - PAD), side)

    brick_c = brick_of(xc, side_c)

    def coarse_w(p, carry):
        r = cr[p]
        place = xc * slab + p - PAD
        keep = both(place >= 0, place < xc * slabs).astype(F32)
        screen = cs[brick_c(p)]
        cw[p] = keep * (screen * r - (cr[p - 1] + cr[p + 1] + sum_c(r, True)))
        return carry

    def coarse_moments(p, acc):
        r, w = cr[p], cw[p]
        image = cs[brick_c(p)] * w - 2.0 * (cw[p + 1] + sum_c(w, False))
        return tuple(a + fold_rows(b) for a, b in zip(acc, (r * r, r * w, w * w, w * image)))

    zero = jnp.zeros((ROWS, LANES), F32)
    lane_index = iota((1, LANES), 1)

    def spread_moments(acc, buf, send, recv, offsets, slot):
        row = jnp.zeros((1, LANES), F32)
        for k, a in enumerate(acc):
            value = jnp.sum(jnp.sum(a, axis=0, keepdims=True), axis=1, keepdims=True)
            row = jnp.where(lane_index == k, value, row)
        buf[slot] = row
        copies = []
        for k, offset in enumerate(offsets):
            c = pltpu.make_async_remote_copy(
                src_ref=buf.at[slot], dst_ref=buf.at[slot], send_sem=send.at[k],
                recv_sem=recv.at[k], device_id=at(offset), device_id_type=MESH,
            )
            c.start()
            copies.append(c)
        return copies

    def solve(copies, buf):
        for c in copies:
            c.wait_recv()
        total = [buf[k] for k in range(buf.shape[0])]
        while len(total) > 1:
            total = [sum(total[k : k + 2][1:], total[k]) for k in range(0, len(total), 2)]
        return coefficients(*[
            jnp.sum(jnp.where(lane_index == k, total[0], 0.0), axis=1, keepdims=True)
            for k in range(4)
        ])

    flat_slot = (ix * ny + iy) * nz + iz
    arrive(near)
    screens(cs, [oc], yc, 0, bc[1], lanes_c, 0)
    lax.fori_loop(PAD, PAD + xc + 1, coarse_w, 0, unroll=True)
    acc = lax.fori_loop(PAD, PAD + xc, coarse_moments, (zero,) * 4, unroll=True)
    coarse_copies = spread_moments(acc, ac, sc, rc, [o for o in peers if o[1] == 0], slab)

    pair_up, made_up = copy(
        edge.at[pl.ds(2, 1)], fb.at[pl.ds(PAD - 1, 1), 0:yf, own_z], above, iz, nz
    )
    pair_dn, made_dn = copy(
        edge.at[pl.ds(0, 2)], fb.at[pl.ds(PAD + xf, 2), 0:yf, own_z], below, iz, nz
    )
    fine_x = [(pair_up, x_high, False), (pair_dn, x_low, False)]
    fine_x += [(c, False, get_low) for c in made_up] + [(c, False, get_high) for c in made_dn]
    start(fine_x)

    arrive(mid_x)
    mid_y = y_swap(mb, xm, ym, 4, 3, 3, m_up, m_dn, m_fu, m_fd)
    start(mid_y)
    arrive(far)
    lax.fori_loop(1, PAD, coarse_w, 0, unroll=True)
    lax.fori_loop(PAD + xc + 1, PAD + xc + 3, coarse_w, 0, unroll=True)
    mid_lanes = lane_prolong(zm, zc)
    mid_rows = row_prolong(ym, ROWS, iy, ym * ny, yc, yc, 0, 0)
    arrive(z_fine)
    fine_flags = x_flags(of, bf[0]) + y_flags(of, of_l, of_r, bf[0])
    start(fine_flags)
    arrive(mid_flags)
    lanes_m = lane_bricks(zm, bm[2], 1)
    screens(ms, [om, om_l, om_r], ym, ROWS, bm[1], lanes_m, 1)

    ka, kb = solve(coarse_copies, ac)
    for j in range(xc + 6):
        cx[j] = ka * cr[j + 1] + kb * cw[j + 1]
    own_c = pl.ds(iz * xc, xc)
    out_c[own_c] = cx[3 : 3 + xc]
    outs = [(copy(out_c.at[own_c], out_c.at[own_c], partner), None, None)]
    start(outs)

    def prolong(src, tz, dst, lane_matrix, row_matrix):
        n, rows, lanes = src.shape
        high, low = split(src[...].reshape(n * rows, lanes))
        tz[...] = (mm(high, lane_matrix) + mm(low, lane_matrix)).reshape(tz.shape)
        for j in range(n):
            high, low = split(tz[j])
            dst[j] = mm(row_matrix, high) + mm(row_matrix, low)

    def interpolate(t, g, own, begin, low, high):
        for p in range(PAD - low, PAD + own + high):
            m = p - PAD
            j = m // 2
            beside = min(max(j + (1 if m % 2 else -1) - begin, 0), t.shape[0] - 1)
            if 0 <= m < own:
                g[p] = 0.75 * t[j - begin] + 0.25 * t[beside]
            else:
                place = own * slab + m
                keep = both(place >= 0, place < own * slabs).astype(F32)
                g[p] = (0.75 * keep) * t[j - begin] + (0.25 * keep) * t[beside]

    def neighbours(v):
        yu, yd = along_y(v)
        return yu + yd + z_up(v) + z_down(v)

    def clear(ref, own, low, high):
        empty = jnp.zeros(ref.shape[1:], F32)

        @pl.when(first)
        def _():
            for p in range(PAD - low, PAD):
                ref[p] = empty

        @pl.when(last)
        def _():
            for p in range(PAD + own, PAD + own + high):
                ref[p] = empty

    def run_depth(b, g, r, w, s, own, rows, index, total, side, r_low, r_high, unroll):
        brick = brick_of(own, side)
        shape = (ROWS, b.shape[2])
        row = logical(iota(shape, 0) + rows, rows, ROWS) + rows * index
        mask = both(row >= 0, row < total).astype(F32)

        def masked(v):
            return jnp.concatenate([v[0:rows], v[rows:] * mask], axis=0)

        def make_r(p, carry):
            c = g[p]
            value = b[p] - (6.0 + s[brick(p)]) * c
            r[p] = masked(value + (g[p - 1] + g[p + 1]) + neighbours(c))
            return carry

        lax.fori_loop(PAD - r_low, PAD + own + r_high, make_r, 0, unroll=unroll)
        clear(r, own, r_low, r_high)

        def make_w(p, carry):
            c = r[p]
            w[p] = masked(s[brick(p)] * c - (r[p - 1] + r[p + 1]) - neighbours(c))
            return carry

        lax.fori_loop(PAD - r_low + 1, PAD + own + r_high - 1, make_w, 0, unroll=unroll)
        clear(w, own, r_low - 1, r_high - 1)

        def moments(p, acc):
            rv, full = r[p, 0:rows], w[p]
            wv = full[0:rows]
            image = s[brick(p), 0:rows] * wv - 2.0 * (
                w[p + 1, 0:rows] + along_y(full)[1][0:rows] + z_down(wv)
            )
            return tuple(
                a + fold_rows(v) for a, v in zip(acc, (rv * rv, rv * wv, wv * wv, wv * image))
            )

        return lax.fori_loop(PAD, PAD + own, moments, (zero,) * 4, unroll=unroll)

    prolong(cx, ctz, ct, mid_lanes, mid_rows)
    interpolate(ct, mg, xm, -3, 4, 4)
    arrive(mid_y)
    y_merge(mb, ym, 4, m_fu, m_fd, 1)
    acc = run_depth(mb, mg, mr, mw, ms, xm, ym, iy, ym * ny, nz * xm // bm[0], 3, 3, 2)
    mid_copies = spread_moments(acc, am, sm, rm, peers, flat_slot)

    arrive(fine_x)
    fine_y = y_swap(fb, xf, yf, 2, 1, 2, f_up, f_dn, f_fu, f_fd)
    start(fine_y)
    arrive(fine_flags)
    lanes_f = lane_bricks(zf, bf[2], nz)
    screens(fs, [of, of_l, of_r], yf, ROWS, bf[1], lanes_f, 2)
    fine_lanes = lane_prolong(zf, zm)
    fine_rows = row_prolong(yf, ROWS, iy, yf * ny, ym + ROWS, ym, ROWS, iy)
    arrive(fine_y)
    y_merge(fb, yf, 2, f_fu, f_fd, PAD - 1)
    ka, kb = solve(mid_copies, am)
    for p in range(2, xm + 6):
        mx[p - 2] = mg[p] + ka * mr[p] + kb * mw[p]
    own_m = pl.ds(iz * xm, xm)
    out_m[own_m] = mx[2 : 2 + xm, 0:ym, :]
    outs.append((copy(out_m.at[own_m], out_m.at[own_m], partner), None, None))
    start(outs[1:])

    prolong(mx, mtz, mt, fine_lanes, fine_rows)
    interpolate(mt, fg, xf, -2, 2, 3)
    acc = run_depth(fb, fg, fr, fw, fs, xf, yf, iy, yf * ny, nz * xf // bf[0], 1, 2, 2)
    fine_copies = spread_moments(acc, af, sf, rf, peers, flat_slot)
    their_z = pl.ds(pl.multiple_of(other * zh, LANES), zh)
    back = [
        (copy(src.at[PAD : PAD + xf, 0:yf, their_z], dst, partner), None, None)
        for src, dst in ((fg, tg), (fr, tr), (fw, tw))
    ]
    start(back)
    for items in (near, far, z_fine, mid_x, mid_flags, fine_x, mid_y, fine_flags, fine_y, outs):
        left(items)
    for c in coarse_copies + mid_copies:
        c.wait_send()
    arrive(outs)
    arrive(back)
    left(back)
    ka, kb = solve(fine_copies, af)
    coef[0] = jnp.broadcast_to(ka, (ROWS, LANES))
    coef[1] = jnp.broadcast_to(kb, (ROWS, LANES))
    for c in fine_copies:
        c.wait_send()


def finish(g, r, w, tg, tr, tw, coef, sol_c, sol_m, out_c, out_m, out_f, buf, sem):
    iz = lax.axis_index("gz")
    xs, yf, zh = tg.shape
    small = [
        pltpu.make_async_copy(sol_c, out_c, sem.at[0]),
        pltpu.make_async_copy(sol_m, out_m, sem.at[1]),
    ]
    for c in small:
        c.start()
    own_z = pl.ds(pl.multiple_of(iz * zh, LANES), zh)
    ka, kb = coef[0, 0:1, 0:1], coef[1, 0:1, 0:1]
    parts = 2
    step = xs // parts
    copies = list(small)
    for part in range(parts):
        for side in range(2):
            place = (iz if side == 0 else 1 - iz) * xs

            def one(x, carry):
                if side == 0:
                    p = x + PAD
                    value = g[p, 0:yf, own_z] + ka * r[p, 0:yf, own_z] + kb * w[p, 0:yf, own_z]
                else:
                    value = tg[x] + ka * tr[x] + kb * tw[x]
                buf[place + x] = value
                return carry

            lax.fori_loop(part * step, part * step + step, one, 0, unroll=2)
            span = pl.ds(place + part * step, step)
            c = pltpu.make_async_copy(buf.at[span], out_f.at[span], sem.at[2 + 2 * part + side])
            c.start()
            copies.append(c)
    for c in copies:
        c.wait()


def shards(dims, *args):
    nx, ny, nz = dims
    rhs_c, rhs_m, rhs_f, occ_c, occ_m, occ_f, _ = args
    xc, yc, zc = rhs_c.shape
    xm, ym, zm = rhs_m.shape
    xf, yf, zh = rhs_f.shape
    zf = zh * nz
    xc, xm, xf = xc // nz, xm // nz, xf // nz
    me, fe = (ym + ROWS, zm), (yf + ROWS, zf)

    def buf(*shape):
        return pltpu.VMEM(shape, F32)

    bm, bf = occ_m.shape[0] + 2, occ_f.shape[0] + 2
    scratch = [
        pltpu.VMEM(a.shape, a.dtype) for a in (rhs_c, rhs_m, rhs_f, occ_c, occ_m, occ_f)
    ]
    scratch += [pltpu.SMEM(args[6].shape, F32), pltpu.SemaphoreType.DMA((7,))]
    scratch += [
        buf(xc + 8, yc, zc), buf(xc + 8, yc, zc), buf(occ_c.shape[0] + 2, yc, zc),
        buf(xc + 6, yc, zc), buf(xc + 6, yc, zm), buf(xc + 6, *me),
        buf(occ_c.shape[0] + 2, ROWS, LANES),
        buf(xm + 8, *me), buf(xm + 8, *me), buf(xm + 8, *me), buf(xm + 8, *me), buf(bm, *me),
        buf(xm + 4, *me), buf(xm + 4, me[0], zf), buf(xm + 4, *fe),
        buf(bm, ROWS, LANES),
        buf(xm + 6, 4, zm), buf(xm + 6, 4, zm), buf(xm + 6, 4, zm), buf(xm + 6, 4, zm),
        buf(bm, ROWS, LANES), buf(bm, ROWS, LANES),
        buf(xf + 8, *fe), buf(bf, *fe), buf(bf, ROWS, nz * LANES),
        buf(xf + 2, yf, zh), buf(3, yf, zh),
        buf(xf + 3, 2, zf), buf(xf + 3, 2, zf), buf(xf + 3, 2, zf), buf(xf + 3, 2, zf),
        buf(bf, ROWS, nz * LANES), buf(bf, ROWS, nz * LANES),
        buf(nx * nz, 1, LANES), buf(nx * ny * nz, 1, LANES), buf(nx * ny * nz, 1, LANES),
    ]
    for count in (48, nx * nz, nx * ny * nz, nx * ny * nz):
        scratch += [pltpu.SemaphoreType.DMA((count,))] * 2
    hbm = pl.BlockSpec(memory_space=pltpu.HBM)
    vmem = pl.BlockSpec(memory_space=pltpu.VMEM)
    field = pltpu.VMEM((xf + 8,) + fe, F32)
    half = pltpu.VMEM((xf, yf, zh), F32)
    made_shapes = [pltpu.VMEM(a.shape, F32) for a in args[:2]]
    made_shapes += [field] * 3 + [half] * 3 + [pltpu.VMEM((2, ROWS, LANES), F32)]
    room = sum(4 * math.prod(a.shape) for a in made_shapes)
    made = pl.pallas_call(
        functools.partial(kernel, dims),
        out_shape=made_shapes,
        in_specs=[hbm] * 7,
        out_specs=[vmem] * 9,
        scratch_shapes=scratch,
        compiler_params=pltpu.CompilerParams(
            collective_id=0, has_side_effects=True, vmem_limit_bytes=VMEM_BYTES - room
        ),
    )(*args)
    sol_c, sol_m, fields = made[0], made[1], made[2:]
    return pl.pallas_call(
        finish,
        out_shape=[jax.ShapeDtypeStruct(a.shape, F32) for a in args[:3]],
        in_specs=[vmem] * 9,
        out_specs=[hbm] * 3,
        scratch_shapes=[pltpu.VMEM(rhs_f.shape, F32), pltpu.SemaphoreType.DMA((6,))],
        compiler_params=pltpu.CompilerParams(vmem_limit_bytes=16 * 1024 * 1024),
    )(*fields, sol_c, sol_m)


def solution(mesh):
    dims = tuple(mesh.shape[axis] for axis in ("gx", "gy", "gz"))
    in_specs = (
        P("gx", None, None), P("gx", "gy", None), P("gx", "gy", "gz"),
        P("gx", None, None), P("gx", "gy", None), P("gx", "gy", "gz"), P(),
    )
    out_specs = (P("gx", None, None), P("gx", "gy", None), P("gx", "gy", "gz"))
    return jax.shard_map(
        functools.partial(shards, dims), mesh=mesh, in_specs=in_specs, out_specs=out_specs,
        check_vma=False,
    )
```

```python
import functools
import math

import jax
import jax.numpy as jnp
from jax import lax
from jax.experimental import pallas as pl
from jax.experimental.pallas import tpu as pltpu
from jax.sharding import PartitionSpec as P

MESH = pl.DeviceIdType.MESH
F32 = jnp.float32
BF16 = jnp.bfloat16
PAD = 4
ROWS = 8
LANES = 128
VMEM_BYTES = 67043328
UNROLL = 2


def iota(shape, dim):
    return lax.broadcasted_iota(jnp.int32, shape, dim)


def logical(index, own, extra):
    if extra == 0:
        return index
    return jnp.where(index < own + extra // 2, index, index - (own + extra))


def prolong_matrix(fine, coarse, total):
    base = lax.shift_right_arithmetic(fine, 1)
    beside = base + 2 * (fine & 1) - 1
    inside = jnp.logical_and(fine >= 0, fine < total)
    value = jnp.where(coarse == base, 0.75, jnp.where(coarse == beside, 0.25, 0.0))
    return jnp.where(inside, value, 0.0).astype(BF16)


def split(values):
    high = values.astype(BF16)
    return high, (values - high.astype(F32)).astype(BF16)


def mm(a, b):
    return jnp.dot(a, b, preferred_element_type=F32)


def fold_rows(values):
    total = values[0:ROWS]
    for row in range(ROWS, values.shape[0], ROWS):
        total = total + values[row : row + ROWS]
    out = total[:, 0:LANES]
    for lane in range(LANES, values.shape[1], LANES):
        out = out + total[:, lane : lane + LANES]
    return out


def coefficients(m0, n1, n2, n3):
    rho = n1 / m0
    spread = n2 - rho * n1
    bent = 6.0 * spread + (n3 - 2.0 * rho * n2 + rho * rho * n1)
    turn = jnp.where(bent > 0.0, jnp.maximum(spread, 0.0) / bent, 0.0)
    first = m0 / ((6.0 + rho) * m0 - jnp.maximum(spread, 0.0) * turn)
    second = -first * turn
    return first - second * rho, second


def kernel(
    dims,
    rhs_c, rhs_m, rhs_f, occ_c, occ_m, occ_f, weight_in,
    out_c, out_m, fg, fr, fw, tg, tr, tw, coef,
    in_c, in_m, in_f, io_c, io_m, io_f, weight, isem,
    cr, cw, cs, ctz, ct, oc,
    mb, g1, g2, u1, u2, v0, v1, v2, ms, mx, mtz, mt, om, m_up, m_dn, m_fu, m_fd, om_l, om_r,
    fb, fs, of, zsend, edge, f_up, f_dn, f_fu, f_fd, of_l, of_r,
    am, af, ss, rs, sm, rm, sf, rf, relay,
):
    nx, ny, nz = dims
    ix, iy, iz = lax.axis_index("gx"), lax.axis_index("gy"), lax.axis_index("gz")
    xc, yc, zc = rhs_c.shape
    xm, ym, zm = rhs_m.shape
    xf, yf, zh = rhs_f.shape
    zf = zh * nz
    xc, xm, xf = xc // nz, xm // nz, xf // nz
    slab = ix * nz + iz
    slabs = nx * nz
    bc, bm, bf = occ_c.shape, occ_m.shape, occ_f.shape
    x_low, x_high = ix > 0, ix < nx - 1
    y_low, y_high = iy > 0, iy < ny - 1
    lower, upper = iz == 0, iz == 1
    first, last = slab == 0, slab == slabs - 1

    def both(a, b):
        return jnp.logical_and(a, b)

    def at(offset):
        return (
            lax.rem(ix + offset[0], nx), lax.rem(iy + offset[1], ny), lax.rem(iz + offset[2], nz)
        )

    for ref in (oc, om, of):
        ref[...] = jnp.zeros_like(ref)

    barrier = pltpu.get_barrier_semaphore()
    peers = [(a, b, c) for a in range(nx) for b in range(ny) for c in range(nz)][1:]
    around = [(a, b) for a in (-1, 1, 0) for b in (-1, 1, 0)]

    def exists(a, b):
        there = [c for c, step in ((x_low, a == -1), (x_high, a == 1), (y_low, b == -1), (y_high, b == 1)) if step]
        return functools.reduce(both, there) if there else None

    def greet(semaphore, a, b, c):
        target = (ix + a, iy + b, c)

        def send():
            pl.semaphore_signal(semaphore, inc=1, device_id=target, device_id_type=MESH)

        there = exists(a, b)
        if there is None:
            send()
        else:
            pl.when(there)(send)

    for a, b in around:
        for c in range(1 if (a, b) == (0, 0) else 0, nz):
            greet(barrier, a, b, lax.rem(iz + c, nz))
    chips = (1 + jnp.where(x_low, 1, 0) + jnp.where(x_high, 1, 0)) * (
        1 + jnp.where(y_low, 1, 0) + jnp.where(y_high, 1, 0)
    )
    rounds = max(nx, ny) - 2

    def relay_send(k):
        if k < rounds:
            for a, b in around[:-1]:
                greet(relay.at[k], a, b, iz)

    def relay_wait(k):
        if k < rounds:
            pl.semaphore_wait(relay.at[k], chips - 1)

    loads = {}
    pairs = (
        ("c", rhs_c, in_c), ("oc", occ_c, io_c), ("w", weight_in, weight), ("f", rhs_f, in_f),
        ("m", rhs_m, in_m), ("om", occ_m, io_m), ("of", occ_f, io_f),
    )
    for k, (name, src, dst) in enumerate(pairs):
        loads[name] = pltpu.make_async_copy(src, dst, isem.at[k])
        loads[name].start()

    @pl.when(first)
    def _():
        cr[0:4] = jnp.zeros((4, yc, zc), F32)
        cs[0] = jnp.zeros((yc, zc), F32)
        for ref in (m_fu, m_fd):
            ref[0:3] = jnp.zeros((3,) + tuple(ref.shape[1:]), F32)
        mb[1:4, 0:ym, :] = jnp.zeros((3, ym, zm), F32)
        fb[2:4, 0:yf, :] = jnp.zeros((2, yf, zf), F32)

    @pl.when(last)
    def _():
        cr[PAD + xc : PAD + xc + 4] = jnp.zeros((4, yc, zc), F32)
        cs[bc[0] + 1] = jnp.zeros((yc, zc), F32)
        for ref in (m_fu, m_fd):
            ref[xm + 3 : xm + 6] = jnp.zeros((3,) + tuple(ref.shape[1:]), F32)
        mb[PAD + xm : PAD + xm + 3, 0:ym, :] = jnp.zeros((3, ym, zm), F32)
        fb[PAD + xf : PAD + xf + 2, 0:yf, :] = jnp.zeros((2, yf, zf), F32)

    @pl.when(jnp.logical_not(x_low))
    def _():
        for ref in (om_l, om_r, of_l, of_r):
            ref[0:1] = jnp.zeros((1,) + tuple(ref.shape[1:]), F32)

    @pl.when(jnp.logical_not(x_high))
    def _():
        for ref in (om_l, om_r, of_l, of_r):
            size = ref.shape[0]
            ref[size - 1 : size] = jnp.zeros((1,) + tuple(ref.shape[1:]), F32)

    @pl.when(jnp.logical_not(y_low))
    def _():
        for ref in (m_fu, f_fu, om_l, of_l):
            ref[...] = jnp.zeros_like(ref)

    @pl.when(jnp.logical_not(y_high))
    def _():
        for ref in (m_fd, f_fd, om_r, of_r):
            ref[...] = jnp.zeros_like(ref)

    loads["c"].wait()
    cr[pl.ds(PAD - 4 * iz, xc + 4)] = in_c[pl.ds(iz * (xc - 4), xc + 4)].astype(F32)
    loads["oc"].wait()
    oc[1 : 1 + bc[0], 0 : bc[1], 0 : bc[2]] = io_c[...].astype(F32)

    pl.semaphore_wait(barrier, chips * nz - 1)
    relay_send(0)

    used = [0]

    def copy(src, dst, target, step=0, count=1):
        k = used[0]
        used[0] += count
        made = [
            pltpu.make_async_remote_copy(
                src_ref=src, dst_ref=dst, send_sem=ss.at[k], recv_sem=rs.at[k + j],
                device_id=target, device_id_type=MESH,
            )
            for j in range(count)
        ]
        if count == 1:
            return made[0]
        sender = pltpu.make_async_remote_copy(
            src_ref=src, dst_ref=dst, send_sem=ss.at[k], recv_sem=rs.at[k + step],
            device_id=target, device_id_type=MESH,
        )
        return sender, made

    def start(items):
        for c, can_send, _ in items:
            if can_send is None:
                c.start()
            elif can_send is not False:
                pl.when(can_send)(c.start)

    def arrive(items):
        for c, _, can_recv in items:
            if can_recv is None:
                c.wait_recv()
            elif can_recv is not False:
                pl.when(can_recv)(c.wait_recv)

    def left(items):
        for c, can_send, _ in items:
            if can_send is None:
                c.wait_send()
            elif can_send is not False:
                pl.when(can_send)(c.wait_send)

    above, below = {"gx": ix + 1, "gz": 0}, {"gx": ix - 1, "gz": 1}
    send_up, get_low = both(upper, x_high), both(lower, x_low)
    send_down, get_high = both(lower, x_low), both(upper, x_high)

    def slab_swap(ref, own, rows, width_low, width_high, skip_low=0, skip_high=0):
        items = []
        stop = PAD + own - skip_low
        items.append((copy(ref.at[stop - width_low : stop, 0:rows, :],
                           ref.at[PAD - skip_low - width_low : PAD - skip_low, 0:rows, :], above),
                      send_up, get_low))
        begin = PAD + skip_high
        items.append((copy(ref.at[begin : begin + width_high, 0:rows, :],
                           ref.at[begin + own : begin + own + width_high, 0:rows, :], below),
                      send_down, get_high))
        return items

    def x_flags(occ, bricks):
        return [
            (copy(occ.at[bricks], occ.at[0], {"gx": ix + 1}), x_high, x_low),
            (copy(occ.at[1], occ.at[bricks + 1], {"gx": ix - 1}), x_low, x_high),
        ]

    def y_flags(occ, occ_l, occ_r, bricks):
        items = []
        flags = pl.ds(1, bricks)
        for dst, step, can_send, can_recv in (
            (occ_l, 1, y_high, y_low), (occ_r, -1, y_low, y_high)
        ):
            items.append((copy(occ.at[flags], dst.at[flags], {"gy": iy + step}), can_send, can_recv))
            items.append((copy(occ.at[bricks], dst.at[0], {"gx": ix + 1, "gy": iy + step}),
                          both(can_send, x_high), both(can_recv, x_low)))
            items.append((copy(occ.at[1], dst.at[bricks + 1], {"gx": ix - 1, "gy": iy + step}),
                          both(can_send, x_low), both(can_recv, x_high)))
        return items

    def y_swap(ref, own, rows, low, high, to_up, to_down, from_low, from_high):
        span = slice(PAD - low, PAD + own + high)
        to_up[...] = ref[span, rows - to_up.shape[1] : rows, :]
        to_down[...] = ref[span, 0 : to_down.shape[1], :]
        return [
            (copy(to_up, from_low, {"gy": iy + 1}), y_high, y_low),
            (copy(to_down, from_high, {"gy": iy - 1}), y_low, y_high),
        ]

    def y_merge(ref, own, from_low, from_high, begin):
        count = from_low.shape[0]
        parts = [from_high[...], from_low[...]]
        gap = ROWS - from_low.shape[1] - from_high.shape[1]
        if gap:
            parts.insert(1, jnp.zeros((count, gap, ref.shape[2]), F32))
        ref[begin : begin + count, own : own + ROWS, :] = jnp.concatenate(parts, axis=1)

    def row_prolong(own, extra, index, total, cols, col_own, col_extra, col_index):
        shape = (own + extra, cols)
        fine = logical(iota(shape, 0), own, extra) + own * index
        coarse = logical(iota(shape, 1), col_own, col_extra) + col_own * col_index
        return prolong_matrix(fine, coarse, total)

    def lane_prolong(cells, rows):
        shape = (rows, cells)
        return prolong_matrix(iota(shape, 1), iota(shape, 0), cells)

    def lane_bricks(cells, bricks, halves):
        shape = (halves * LANES, cells)
        brick = lax.div(iota(shape, 1), cells // (bricks * halves))
        place = brick + lax.div(brick, bricks) * (LANES - bricks)
        return (place == iota(shape, 0)).astype(BF16)

    def screens(dest, begin, count, occ_parts, own, extra_rows, bricks_y, lane_matrix, level):
        side = own // bricks_y
        cols = ROWS * len(occ_parts)
        shape = (dest.shape[1], cols)
        brick = lax.div(logical(iota(shape, 0), own, extra_rows) + side, side) - 1
        place = jnp.where(
            brick < 0, ROWS + bricks_y - 1, jnp.where(brick >= bricks_y, 2 * ROWS, brick)
        )
        row_matrix = (place == iota(shape, 1)).astype(BF16)
        flags = [part[begin + x] for x in range(count) for part in occ_parts]
        wide = mm(jnp.concatenate(flags, axis=0).astype(BF16), lane_matrix).astype(BF16)
        for x in range(count):
            cells = mm(row_matrix, wide[x * cols : (x + 1) * cols])
            dest[begin + x] = weight[level] * (0.25 + cells)

    near = slab_swap(cr, xc, yc, 1, 2)
    start(near)
    loads["w"].wait()
    screens(cs, 1, bc[0], [oc], yc, 0, bc[1], lane_bricks(zc, bc[2], 1), 0)
    near_screens = [
        (copy(cs.at[bc[0]], cs.at[0], above), send_up, get_low),
        (copy(cs.at[1], cs.at[bc[0] + 1], below), send_down, get_high),
    ]
    start(near_screens)
    far = slab_swap(cr, xc, yc, 3, 2, 1, 2)
    start(far)

    loads["m"].wait()
    mb[pl.ds(PAD - 3 * iz, xm + 3), 0:ym, :] = in_m[pl.ds(iz * (xm - 3), xm + 3)].astype(F32)
    loads["om"].wait()
    om[1 : 1 + bm[0], 0 : bm[1], 0 : bm[2]] = io_m[...].astype(F32)
    mid_flags = x_flags(om, bm[0]) + y_flags(om, om_l, om_r, bm[0])
    start(mid_flags)
    mid_x = slab_swap(mb, xm, ym, 3, 3)
    start(mid_x)
    held = pl.ds(3 - 3 * iz, xm + 3)
    m_up[held] = mb[pl.ds(PAD - 3 * iz, xm + 3), ym - 4 : ym, :]
    m_dn[held] = mb[pl.ds(PAD - 3 * iz, xm + 3), 0:4, :]
    mid_y = []
    for src, dst, step, can_send, can_recv in (
        (m_up, m_fu, 1, y_high, y_low), (m_dn, m_fd, -1, y_low, y_high)
    ):
        side = {"gy": iy + step}
        mid_y.append((copy(src.at[held], dst.at[held], side), can_send, can_recv))
        mid_y.append((copy(src.at[xm : xm + 3], dst.at[0:3], {**above, **side}),
                      both(can_send, send_up), both(can_recv, get_low)))
        mid_y.append((copy(src.at[3:6], dst.at[xm + 3 : xm + 6], {**below, **side}),
                      both(can_send, send_down), both(can_recv, get_high)))
    start(mid_y)

    loads["f"].wait()
    own_z = pl.ds(pl.multiple_of(iz * zh, LANES), zh)
    other = 1 - iz

    def fill_fine(j, carry):
        zsend[j] = in_f[other * (xf - 2) + j].astype(F32)
        fb[PAD - 2 * iz + j, 0:yf, own_z] = in_f[iz * (xf - 2) + j].astype(F32)
        return carry

    lax.fori_loop(0, xf + 2, fill_fine, 0)
    loads["of"].wait()
    own_flags = pl.ds(pl.multiple_of(iz * LANES, LANES), LANES)
    flags = jnp.concatenate(
        [io_f[...].astype(F32), jnp.zeros((bf[0], bf[1], LANES - bf[2]), F32)], axis=2
    )
    of[1 : 1 + bf[0], 0 : bf[1], own_flags] = flags
    partner = {"gz": other}
    z_fine = [
        (copy(zsend, fb.at[pl.ds(PAD - 2 * other, xf + 2), 0:yf, own_z], partner), None, None),
        (copy(of.at[pl.ds(1, bf[0]), :, own_flags], of.at[pl.ds(1, bf[0]), :, own_flags], partner),
         None, None),
    ]
    start(z_fine)

    edge[0:2] = in_f[0:2].astype(F32)
    edge[2] = in_f[nz * xf - 1].astype(F32)
    pair_up, made_up = copy(
        edge.at[pl.ds(2, 1)], fb.at[pl.ds(PAD - 1, 1), 0:yf, own_z], above, iz, nz
    )
    pair_dn, made_dn = copy(
        edge.at[pl.ds(0, 2)], fb.at[pl.ds(PAD + xf, 2), 0:yf, own_z], below, iz, nz
    )
    fine_x = [(pair_up, x_high, False), (pair_dn, x_low, False)]
    fine_x += [(c, False, get_low) for c in made_up] + [(c, False, get_high) for c in made_dn]
    start(fine_x)

    def along_y(v):
        n = v.shape[0]
        return pltpu.roll(v, 1, 0), pltpu.roll(v, n - 1, 0)

    def z_up(v):
        n = v.shape[1]
        turned = pltpu.roll(v, 1, 1)
        edge_lane = iota((v.shape[0], LANES), 1) == 0
        fixed = jnp.where(edge_lane, 0.0, turned[:, 0:LANES])
        return fixed if n == LANES else jnp.concatenate([fixed, turned[:, LANES:]], axis=1)

    def z_down(v):
        n = v.shape[1]
        turned = pltpu.roll(v, n - 1, 1)
        edge_lane = iota((v.shape[0], LANES), 1) == LANES - 1
        fixed = jnp.where(edge_lane, 0.0, turned[:, n - LANES :])
        return fixed if n == LANES else jnp.concatenate([turned[:, : n - LANES], fixed], axis=1)

    side_c = nz * xc // bc[0]
    shape_c = (yc, zc)
    row_c = iota(shape_c, 0)

    def sum_c(v, twice):
        yu, yd = along_y(v)
        total = jnp.where(row_c < yc - 1, yd, 0.0) + z_down(v)
        if twice:
            total = total + jnp.where(row_c > 0, yu, 0.0) + z_up(v)
        return total

    def brick_of(own, side):
        return lambda p: lax.div(own * iz + p + (side - PAD), side)

    brick_c = brick_of(xc, side_c)

    def coarse_w(p, carry):
        r = cr[p]
        place = xc * slab + p - PAD
        keep = both(place >= 0, place < xc * slabs).astype(F32)
        screen = cs[brick_c(p)]
        cw[p] = keep * (screen * r - (cr[p - 1] + cr[p + 1] + sum_c(r, True)))
        return carry

    def coarse_moments(p, acc):
        r, w = cr[p], cw[p]
        image = cs[brick_c(p)] * w - 2.0 * (cw[p + 1] + sum_c(w, False))
        return tuple(a + fold_rows(b) for a, b in zip(acc, (r * r, r * w, w * w, w * image)))

    zero = jnp.zeros((ROWS, LANES), F32)
    lane_index = iota((1, LANES), 1)

    def spread_moments(values, buf, send, recv):
        row = jnp.zeros((1, LANES), F32)
        for k, a in values:
            value = jnp.sum(jnp.sum(a, axis=0, keepdims=True), axis=1, keepdims=True)
            row = jnp.where(lane_index == k, value, row)
        slot = (ix * ny + iy) * nz + iz
        buf[slot] = row
        copies = []
        for k, offset in enumerate(peers):
            c = pltpu.make_async_remote_copy(
                src_ref=buf.at[slot], dst_ref=buf.at[slot], send_sem=send.at[k],
                recv_sem=recv.at[k], device_id=at(offset), device_id_type=MESH,
            )
            c.start()
            copies.append(c)
        return copies

    def gathered(copies, buf):
        for c in copies:
            c.wait_recv()
        total = [buf[k] for k in range(buf.shape[0])]
        while len(total) > 1:
            total = [sum(total[k : k + 2][1:], total[k]) for k in range(0, len(total), 2)]
        return total[0]

    def picked(row, test):
        return jnp.sum(jnp.where(test, row, 0.0), axis=1, keepdims=True)

    def prolong(values, tz, dst, lane_matrix, row_matrix):
        n, rows, lanes = values.shape
        high, low = split(values.reshape(n * rows, lanes))
        tz[...] = (mm(high, lane_matrix) + mm(low, lane_matrix)).reshape(tz.shape)
        twice = jnp.concatenate([row_matrix, row_matrix], axis=1)
        for j in range(n):
            dst[j] = mm(twice, jnp.concatenate(split(tz[j]), axis=0))

    def interpolate(t, g, own, begin, low, high):
        for p in range(PAD - low, PAD + own + high):
            m = p - PAD
            j = m // 2
            beside = min(max(j + (1 if m % 2 else -1) - begin, 0), t.shape[0] - 1)
            if 0 <= m < own:
                g[p] = 0.75 * t[j - begin] + 0.25 * t[beside]
            else:
                place = own * slab + m
                keep = both(place >= 0, place < own * slabs).astype(F32)
                g[p] = (0.75 * keep) * t[j - begin] + (0.25 * keep) * t[beside]

    def neighbours(v):
        yu, yd = along_y(v)
        return yu + yd + z_up(v) + z_down(v)

    def clear(ref, own, low, high):
        empty = jnp.zeros(ref.shape[1:], F32)

        @pl.when(first)
        def _():
            for p in range(PAD - low, PAD):
                ref[p] = empty

        @pl.when(last)
        def _():
            for p in range(PAD + own, PAD + own + high):
                ref[p] = empty

    def row_mask(rows, index, total, lanes):
        shape = (ROWS, lanes)
        row = logical(iota(shape, 0) + rows, rows, ROWS) + rows * index
        return both(row >= 0, row < total).astype(F32)

    def masked(v, mask):
        rows = v.shape[0] - ROWS
        return jnp.concatenate([v[0:rows], v[rows:] * mask], axis=0)

    def upward(ref, p, full, rows):
        return ref[p + 1, 0:rows] + along_y(full)[1][0:rows] + z_down(full[0:rows])

    arrive(near)
    arrive(near_screens)
    relay_wait(0)
    relay_send(1)
    lax.fori_loop(PAD, PAD + xc + 1, coarse_w, 0, unroll=True)
    acc_c = lax.fori_loop(PAD, PAD + xc, coarse_moments, (zero,) * 4, unroll=True)
    mid_lanes = lane_prolong(zm, zc)
    mid_rows = row_prolong(ym, ROWS, iy, ym * ny, yc, yc, 0, 0)
    arrive(far)
    prolong(cr[1 : xc + 7], ctz, ct, mid_lanes, mid_rows)
    interpolate(ct, g1, xm, -3, 4, 4)
    lax.fori_loop(1, PAD, coarse_w, 0, unroll=True)
    lax.fori_loop(PAD + xc + 1, PAD + xc + 3, coarse_w, 0, unroll=True)
    prolong(cw[1 : xc + 7], ctz, ct, mid_lanes, mid_rows)
    interpolate(ct, g2, xm, -3, 4, 4)
    arrive(mid_flags)
    screens(ms, 0, bm[0] + 2, [om, om_l, om_r], ym, ROWS, bm[1], lane_bricks(zm, bm[2], 1), 1)
    mask_m = row_mask(ym, iy, ym * ny, zm)
    brick_m = brick_of(xm, nz * xm // bm[0])

    def mid_u(p, carry):
        screen = 6.0 + ms[brick_m(p)]
        for g, u in ((g1, u1), (g2, u2)):
            c = g[p]
            u[p] = masked(screen * c - (g[p - 1] + g[p + 1]) - neighbours(c), mask_m)
        return carry

    lax.fori_loop(PAD - 3, PAD + xm + 3, mid_u, 0, unroll=True)
    for ref in (u1, u2):
        clear(ref, xm, 3, 3)
    arrive(mid_x)
    arrive(mid_y)
    y_merge(mb, ym, m_fu, m_fd, 1)
    fields = ((mb, v0), (u1, v1), (u2, v2))

    def mid_v(p, carry):
        screen = ms[brick_m(p)]
        for u, v in fields:
            c = u[p]
            v[p] = masked(screen * c - (u[p - 1] + u[p + 1]) - neighbours(c), mask_m)
        return carry

    lax.fori_loop(PAD - 2, PAD + xm + 2, mid_v, 0, unroll=True)
    for ref in (v0, v1, v2):
        clear(ref, xm, 2, 2)
    pairs_m = ((0, 0), (1, 1), (2, 2), (0, 1), (0, 2), (1, 2))

    def mid_moments(p, acc):
        screen = ms[brick_m(p), 0:ym]
        us = [u[p, 0:ym] for u, _ in fields]
        full = [v[p] for _, v in fields]
        vs = [v[0:ym] for v in full]
        images = [
            screen * v - 2.0 * upward(ref, p, f, ym) for v, f, (_, ref) in zip(vs, full, fields)
        ]
        values = [us[i] * us[j] for i, j in pairs_m] + [us[i] * vs[j] for i, j in pairs_m]
        values += [vs[i] * vs[j] for i, j in pairs_m]
        for i, j in pairs_m:
            cross = vs[i] * images[j]
            values.append(cross if i == j else 0.5 * (cross + vs[j] * images[i]))
        return tuple(a + fold_rows(v) for a, v in zip(acc, values))

    acc = lax.fori_loop(PAD, PAD + xm, mid_moments, (zero,) * 24, unroll=2)
    relay_wait(1)
    for k in range(2, rounds):
        relay_send(k)
        relay_wait(k)
    slots = [(ROWS * (k // 6) + k % 6, a) for k, a in enumerate(acc)]
    slots += [(4 * ROWS + k, a) for k, a in enumerate(acc_c)]
    mid_copies = spread_moments(slots, am, sm, rm)

    arrive(z_fine)
    fine_flags = x_flags(of, bf[0]) + y_flags(of, of_l, of_r, bf[0])
    start(fine_flags)
    arrive(fine_x)
    fine_y = y_swap(fb, xf, yf, 1, 2, f_up, f_dn, f_fu, f_fd)
    start(fine_y)
    arrive(fine_flags)
    lanes_f = lane_bricks(zf, bf[2], nz)
    screens(fs, 0, bf[0] + 2, [of, of_l, of_r], yf, ROWS, bf[1], lanes_f, 2)
    fine_lanes = lane_prolong(zf, zm)
    fine_rows = row_prolong(yf, ROWS, iy, yf * ny, ym + ROWS, ym, ROWS, iy)
    arrive(fine_y)
    y_merge(fb, yf, f_fu, f_fd, PAD - 1)
    total = gathered(mid_copies, am)
    ka, kb = coefficients(*[picked(total, lane_index == 4 * ROWS + k) for k in range(4)])
    weights = [None, ka * ka, kb * kb, -2.0 * ka, -2.0 * kb, 2.0 * ka * kb]
    kind = lane_index % ROWS
    scaled = total
    for k in range(1, 6):
        scaled = jnp.where(kind == k, total * weights[k], scaled)
    place = lax.div(lane_index, ROWS)
    km, kw = coefficients(*[
        picked(scaled, both(place == k, kind < 6)) for k in range(4)
    ])
    parts = (
        (g1, ka), (g2, kb), (mb, km), (u1, -km * ka), (u2, -km * kb),
        (v0, kw), (v1, -kw * ka), (v2, -kw * kb),
    )
    for p in range(2, xm + 6):
        value = parts[0][1] * parts[0][0][p]
        for ref, factor in parts[1:]:
            value = value + factor * ref[p]
        mx[p - 2] = value
    own_c, own_m = pl.ds(iz * xc, xc), pl.ds(iz * xm, xm)

    prolong(mx[...], mtz, mt, fine_lanes, fine_rows)
    interpolate(mt, fg, xf, -2, 2, 3)
    brick_f = brick_of(xf, nz * xf // bf[0])
    mask_f = row_mask(yf, iy, yf * ny, zf)

    def make_r(p, carry):
        c = fg[p]
        value = fb[p] - (6.0 + fs[brick_f(p)]) * c
        fr[p] = masked(value + (fg[p - 1] + fg[p + 1]) + neighbours(c), mask_f)
        return carry

    lax.fori_loop(PAD - 1, PAD + xf + 2, make_r, 0, unroll=UNROLL)
    clear(fr, xf, 1, 2)

    def make_w(p, carry):
        c = fr[p]
        fw[p] = masked(fs[brick_f(p)] * c - (fr[p - 1] + fr[p + 1]) - neighbours(c), mask_f)
        return carry

    lax.fori_loop(PAD, PAD + xf + 1, make_w, 0, unroll=UNROLL)
    clear(fw, xf, 0, 1)

    def moments(p, acc):
        rv, full = fr[p, 0:yf], fw[p]
        wv = full[0:yf]
        image = fs[brick_f(p), 0:yf] * wv - 2.0 * upward(fw, p, full, yf)
        return tuple(
            a + fold_rows(v) for a, v in zip(acc, (rv * rv, rv * wv, wv * wv, wv * image))
        )

    acc = lax.fori_loop(PAD, PAD + xf, moments, (zero,) * 4, unroll=UNROLL)
    fine_copies = spread_moments(list(enumerate(acc)), af, sf, rf)
    their_z = pl.ds(pl.multiple_of(other * zh, LANES), zh)
    back = [
        (copy(src.at[PAD : PAD + xf, 0:yf, their_z], dst, partner), None, None)
        for src, dst in ((fg, tg), (fr, tr), (fw, tw))
    ]
    start(back)
    out_c[own_c] = ka * cr[PAD : PAD + xc] + kb * cw[PAD : PAD + xc]
    out_m[own_m] = mx[2 : 2 + xm, 0:ym, :]
    outs = [
        (copy(out_c.at[own_c], out_c.at[own_c], partner), None, None),
        (copy(out_m.at[own_m], out_m.at[own_m], partner), None, None),
    ]
    start(outs)
    for items in (
        near, near_screens, far, z_fine, mid_x, mid_flags, fine_x, mid_y, fine_flags, fine_y, outs
    ):
        left(items)
    for c in mid_copies:
        c.wait_send()
    arrive(outs)
    arrive(back)
    left(back)
    total = gathered(fine_copies, af)
    ka, kb = coefficients(*[picked(total, lane_index == k) for k in range(4)])
    coef[0] = jnp.broadcast_to(ka, (ROWS, LANES))
    coef[1] = jnp.broadcast_to(kb, (ROWS, LANES))
    for c in fine_copies:
        c.wait_send()


def finish(g, r, w, tg, tr, tw, coef, sol_c, sol_m, out_c, out_m, out_f, buf, sem):
    iz = lax.axis_index("gz")
    xs, yf, zh = tg.shape
    small = [
        pltpu.make_async_copy(sol_c, out_c, sem.at[0]),
        pltpu.make_async_copy(sol_m, out_m, sem.at[1]),
    ]
    for c in small:
        c.start()
    own_z = pl.ds(pl.multiple_of(iz * zh, LANES), zh)
    ka, kb = coef[0, 0:1, 0:1], coef[1, 0:1, 0:1]
    parts = 2
    step = xs // parts
    copies = list(small)
    for part in range(parts):
        for side in range(2):
            place = (iz if side == 0 else 1 - iz) * xs

            def one(x, carry):
                if side == 0:
                    p = x + PAD
                    value = g[p, 0:yf, own_z] + ka * r[p, 0:yf, own_z] + kb * w[p, 0:yf, own_z]
                else:
                    value = tg[x] + ka * tr[x] + kb * tw[x]
                buf[place + x] = value
                return carry

            lax.fori_loop(part * step, part * step + step, one, 0, unroll=2)
            span = pl.ds(place + part * step, step)
            c = pltpu.make_async_copy(buf.at[span], out_f.at[span], sem.at[2 + 2 * part + side])
            c.start()
            copies.append(c)
    for c in copies:
        c.wait()


def shards(dims, *args):
    nx, ny, nz = dims
    rhs_c, rhs_m, rhs_f, occ_c, occ_m, occ_f, _ = args
    xc, yc, zc = rhs_c.shape
    xm, ym, zm = rhs_m.shape
    xf, yf, zh = rhs_f.shape
    zf = zh * nz
    xc, xm, xf = xc // nz, xm // nz, xf // nz
    me, fe = (ym + ROWS, zm), (yf + ROWS, zf)

    def buf(*shape):
        return pltpu.VMEM(shape, F32)

    bm, bf = occ_m.shape[0] + 2, occ_f.shape[0] + 2
    scratch = [
        pltpu.VMEM(a.shape, a.dtype) for a in (rhs_c, rhs_m, rhs_f, occ_c, occ_m, occ_f)
    ]
    scratch += [pltpu.SMEM(args[6].shape, F32), pltpu.SemaphoreType.DMA((7,))]
    scratch += [
        buf(xc + 8, yc, zc), buf(xc + 8, yc, zc), buf(occ_c.shape[0] + 2, yc, zc),
        buf(xc + 6, yc, zm), buf(xc + 6, *me),
        buf(occ_c.shape[0] + 2, ROWS, LANES),
    ]
    scratch += [buf(xm + 8, *me)] * 8
    scratch += [
        buf(bm, *me),
        buf(xm + 4, *me), buf(xm + 4, me[0], zf), buf(xm + 4, *fe),
        buf(bm, ROWS, LANES),
        buf(xm + 6, 4, zm), buf(xm + 6, 4, zm), buf(xm + 6, 4, zm), buf(xm + 6, 4, zm),
        buf(bm, ROWS, LANES), buf(bm, ROWS, LANES),
        buf(xf + 8, *fe), buf(bf, *fe), buf(bf, ROWS, nz * LANES),
        buf(xf + 2, yf, zh), buf(3, yf, zh),
        buf(xf + 3, 1, zf), buf(xf + 3, 2, zf), buf(xf + 3, 1, zf), buf(xf + 3, 2, zf),
        buf(bf, ROWS, nz * LANES), buf(bf, ROWS, nz * LANES),
        buf(nx * ny * nz, 1, LANES), buf(nx * ny * nz, 1, LANES),
    ]
    for count in (64, nx * ny * nz, nx * ny * nz):
        scratch += [pltpu.SemaphoreType.DMA((count,))] * 2
    scratch += [pltpu.SemaphoreType.REGULAR((max(nx, ny),))]
    hbm = pl.BlockSpec(memory_space=pltpu.HBM)
    vmem = pl.BlockSpec(memory_space=pltpu.VMEM)
    field = pltpu.VMEM((xf + 8,) + fe, F32)
    half = pltpu.VMEM((xf, yf, zh), F32)
    made_shapes = [pltpu.VMEM(a.shape, F32) for a in args[:2]]
    made_shapes += [field] * 3 + [half] * 3 + [pltpu.VMEM((2, ROWS, LANES), F32)]
    room = sum(4 * math.prod(a.shape) for a in made_shapes)
    made = pl.pallas_call(
        functools.partial(kernel, dims),
        out_shape=made_shapes,
        in_specs=[hbm] * 7,
        out_specs=[vmem] * 9,
        scratch_shapes=scratch,
        compiler_params=pltpu.CompilerParams(
            collective_id=0, has_side_effects=True, vmem_limit_bytes=VMEM_BYTES - room
        ),
    )(*args)
    sol_c, sol_m, fields = made[0], made[1], made[2:]
    return pl.pallas_call(
        finish,
        out_shape=[jax.ShapeDtypeStruct(a.shape, F32) for a in args[:3]],
        in_specs=[vmem] * 9,
        out_specs=[hbm] * 3,
        scratch_shapes=[pltpu.VMEM(rhs_f.shape, F32), pltpu.SemaphoreType.DMA((6,))],
        compiler_params=pltpu.CompilerParams(vmem_limit_bytes=16 * 1024 * 1024),
    )(*fields, sol_c, sol_m)


def solution(mesh):
    dims = tuple(mesh.shape[axis] for axis in ("gx", "gy", "gz"))
    in_specs = (
        P("gx", None, None), P("gx", "gy", None), P("gx", "gy", "gz"),
        P("gx", None, None), P("gx", "gy", None), P("gx", "gy", "gz"), P(),
    )
    out_specs = (P("gx", None, None), P("gx", "gy", None), P("gx", "gy", "gz"))
    return jax.shard_map(
        functools.partial(shards, dims), mesh=mesh, in_specs=in_specs, out_specs=out_specs,
        check_vma=False,
    )
```

```python
import functools
import math

import jax
import jax.numpy as jnp
from jax import lax
from jax.experimental import pallas as pl
from jax.experimental.pallas import tpu as pltpu
from jax.sharding import PartitionSpec as P

MESH = pl.DeviceIdType.MESH
F32 = jnp.float32
BF16 = jnp.bfloat16
PAD = 4
ROWS = 8
TOP = 8
LANES = 128
VMEM_BYTES = 67043328
UNROLL = True


def iota(shape, dim):
    return lax.broadcasted_iota(jnp.int32, shape, dim)


def prolong_matrix(fine, coarse, total):
    base = lax.shift_right_arithmetic(fine, 1)
    beside = base + 2 * (fine & 1) - 1
    inside = jnp.logical_and(fine >= 0, fine < total)
    value = jnp.where(coarse == base, 0.75, jnp.where(coarse == beside, 0.25, 0.0))
    return jnp.where(inside, value, 0.0).astype(BF16)


def split(values):
    high = values.astype(BF16)
    return high, (values - high.astype(F32)).astype(BF16)


def mm(a, b):
    return jnp.dot(a, b, preferred_element_type=F32)


def fold_rows(values):
    total = values[0:ROWS]
    for row in range(ROWS, values.shape[0], ROWS):
        total = total + values[row : row + ROWS]
    out = total[:, 0:LANES]
    for lane in range(LANES, values.shape[1], LANES):
        out = out + total[:, lane : lane + LANES]
    return out


def coefficients(m0, n1, n2, n3):
    rho = n1 / m0
    spread = n2 - rho * n1
    bent = 6.0 * spread + (n3 - 2.0 * rho * n2 + rho * rho * n1)
    turn = jnp.where(bent > 0.0, jnp.maximum(spread, 0.0) / bent, 0.0)
    first = m0 / ((6.0 + rho) * m0 - jnp.maximum(spread, 0.0) * turn)
    second = -first * turn
    return first - second * rho, second


def kernel(
    dims,
    rhs_c, rhs_m, rhs_f, occ_c, occ_m, occ_f, weight_in,
    out_c, out_m, fg, fr, fw, tg, tr, tw, coef,
    in_c, in_m, in_f, io_c, io_m, io_f, weight, isem,
    cr, cw, cs, ctz, ct, oc,
    mb, g1, g2, u1, u2, v0, v1, v2, ms, mx, mtz, mt, om, m_up, m_dn, m_fu, m_fd, om_l, om_r,
    fb, fs, of, zsend, edge, f_up, f_dn, f_fu, f_fd, of_l, of_r,
    am, af, ss, rs, sm, rm, sf, rf, relay,
):
    nx, ny, nz = dims
    ix, iy, iz = lax.axis_index("gx"), lax.axis_index("gy"), lax.axis_index("gz")
    xc, yc, zc = rhs_c.shape
    xm, ym, zm = rhs_m.shape
    xf, yf, zh = rhs_f.shape
    zf = zh * nz
    xc, xm, xf = xc // nz, xm // nz, xf // nz
    cm, cf, ch = zm // LANES, zf // LANES, zh // LANES
    slab = ix * nz + iz
    slabs = nx * nz
    bc, bm, bf = occ_c.shape, occ_m.shape, occ_f.shape
    x_low, x_high = ix > 0, ix < nx - 1
    y_low, y_high = iy > 0, iy < ny - 1
    lower, upper = iz == 0, iz == 1
    first, last = slab == 0, slab == slabs - 1
    rows_c, rows_m, rows_f = (slice(TOP, TOP + n) for n in (yc, ym, yf))

    def both(a, b):
        return jnp.logical_and(a, b)

    def at(offset):
        return (
            lax.rem(ix + offset[0], nx), lax.rem(iy + offset[1], ny), lax.rem(iz + offset[2], nz)
        )

    loads = {}
    pairs = (
        ("c", rhs_c, in_c), ("oc", occ_c, io_c), ("om", occ_m, io_m), ("w", weight_in, weight),
        ("m", rhs_m, in_m), ("f", rhs_f, in_f), ("of", occ_f, io_f),
    )
    for k, (name, src, dst) in enumerate(pairs):
        loads[name] = pltpu.make_async_copy(src, dst, isem.at[k])
        loads[name].start()

    for ref in (oc, om, of):
        ref[...] = jnp.zeros_like(ref)

    barrier = pltpu.get_barrier_semaphore()
    peers = [(a, b, c) for a in range(nx) for b in range(ny) for c in range(nz)][1:]
    around = [(a, b) for a in (-1, 1, 0) for b in (-1, 1, 0)]

    def greet(semaphore, a, b, c):
        def send():
            pl.semaphore_signal(
                semaphore, inc=1, device_id=(ix + a, iy + b, c), device_id_type=MESH
            )

        tests = ((x_low, a < 0), (x_high, a > 0), (y_low, b < 0), (y_high, b > 0))
        there = [test for test, needed in tests if needed]
        if there:
            pl.when(functools.reduce(both, there))(send)
        else:
            send()

    for a, b in around:
        for c in range(1 if (a, b) == (0, 0) else 0, nz):
            greet(barrier, a, b, lax.rem(iz + c, nz))
    chips = (1 + jnp.where(x_low, 1, 0) + jnp.where(x_high, 1, 0)) * (
        1 + jnp.where(y_low, 1, 0) + jnp.where(y_high, 1, 0)
    )
    rounds = max(nx, ny) - 2

    def relay_send(k):
        if k < rounds:
            for a, b in around[:-1]:
                greet(relay.at[k], a, b, iz)

    def relay_wait(k):
        if k < rounds:
            pl.semaphore_wait(relay.at[k], chips - 1)

    def wipe(ref, planes):
        for p in planes:
            ref[p] = jnp.zeros(tuple(ref.shape[1:]), F32)

    @pl.when(first)
    def _():
        wipe(cr, range(0, 4))
        wipe(cs, (0,))
        wipe(mb, range(1, 4))
        wipe(fb, range(2, 4))
        for ref in (m_fu, m_fd):
            wipe(ref, range(0, 3))

    @pl.when(last)
    def _():
        wipe(cr, range(PAD + xc, PAD + xc + 4))
        wipe(cs, (bc[0] + 1,))
        wipe(mb, range(PAD + xm, PAD + xm + 3))
        wipe(fb, range(PAD + xf, PAD + xf + 2))
        for ref in (m_fu, m_fd):
            wipe(ref, range(xm + 3, xm + 6))

    @pl.when(jnp.logical_not(x_low))
    def _():
        for ref in (om_l, om_r, of_l, of_r):
            wipe(ref, (0,))

    @pl.when(jnp.logical_not(x_high))
    def _():
        for ref in (om_l, om_r, of_l, of_r):
            wipe(ref, (ref.shape[0] - 1,))

    @pl.when(jnp.logical_not(y_low))
    def _():
        for ref in (m_fu, f_fu, om_l, of_l):
            ref[...] = jnp.zeros_like(ref)

    @pl.when(jnp.logical_not(y_high))
    def _():
        for ref in (m_fd, f_fd, om_r, of_r):
            ref[...] = jnp.zeros_like(ref)

    loads["oc"].wait()
    oc[1 : 1 + bc[0], 0 : bc[1], 0 : bc[2]] = io_c[...].astype(F32)
    loads["om"].wait()
    om[1 : 1 + bm[0], 0 : bm[1], 0 : bm[2]] = io_m[...].astype(F32)
    loads["c"].wait()
    cr[pl.ds(PAD - 4 * iz, xc + 4), rows_c] = in_c[pl.ds(iz * (xc - 4), xc + 4)].astype(F32)

    pl.semaphore_wait(barrier, chips * nz - 1)
    relay_send(0)

    used = [0]

    def copy(src, dst, target, step=0, count=1):
        k = used[0]
        used[0] += count

        def made(j):
            return pltpu.make_async_remote_copy(
                src_ref=src, dst_ref=dst, send_sem=ss.at[k], recv_sem=rs.at[k + j],
                device_id=target, device_id_type=MESH,
            )

        return made(0) if count == 1 else (made(step), [made(j) for j in range(count)])

    def start(items):
        for c, can_send, _ in items:
            if can_send is None:
                c.start()
            elif can_send is not False:
                pl.when(can_send)(c.start)

    def arrive(items):
        for c, _, can_recv in items:
            if can_recv is None:
                c.wait_recv()
            elif can_recv is not False:
                pl.when(can_recv)(c.wait_recv)

    def left(items):
        for c, can_send, _ in items:
            if can_send is None:
                c.wait_send()
            elif can_send is not False:
                pl.when(can_send)(c.wait_send)

    above, below = {"gx": ix + 1, "gz": 0}, {"gx": ix - 1, "gz": 1}
    send_up, get_low = both(upper, x_high), both(lower, x_low)
    send_down, get_high = both(lower, x_low), both(upper, x_high)

    def slab_swap(view, own, width_low, width_high, skip_low=0, skip_high=0):
        stop, begin = PAD + own - skip_low, PAD + skip_high
        low = PAD - skip_low - width_low
        return [
            (copy(view(stop - width_low, width_low), view(low, width_low), above),
             send_up, get_low),
            (copy(view(begin, width_high), view(begin + own, width_high), below),
             send_down, get_high),
        ]

    def x_flags(occ, bricks):
        return [
            (copy(occ.at[bricks], occ.at[0], {"gx": ix + 1}), x_high, x_low),
            (copy(occ.at[1], occ.at[bricks + 1], {"gx": ix - 1}), x_low, x_high),
        ]

    def y_flags(occ, occ_l, occ_r, bricks):
        items = []
        flags = pl.ds(1, bricks)
        for dst, step, can_send, can_recv in (
            (occ_l, 1, y_high, y_low), (occ_r, -1, y_low, y_high)
        ):
            items.append((copy(occ.at[flags], dst.at[flags], {"gy": iy + step}), can_send, can_recv))
            items.append((copy(occ.at[bricks], dst.at[0], {"gx": ix + 1, "gy": iy + step}),
                          both(can_send, x_high), both(can_recv, x_low)))
            items.append((copy(occ.at[1], dst.at[bricks + 1], {"gx": ix - 1, "gy": iy + step}),
                          both(can_send, x_low), both(can_recv, x_high)))
        return items

    def row_prolong(own, margin, index, total, cols, col_first):
        shape = (own + ROWS, cols)
        fine = iota(shape, 0) - margin + own * index
        return prolong_matrix(fine, iota(shape, 1) + col_first, total)

    def lane_prolong(cells, rows):
        shape = (rows, cells)
        return prolong_matrix(iota(shape, 1), iota(shape, 0), cells)

    def lane_bricks(cells, bricks, halves):
        shape = (halves * LANES, cells)
        brick = lax.div(iota(shape, 1), cells // (bricks * halves))
        place = brick + lax.div(brick, bricks) * (LANES - bricks)
        return (place == iota(shape, 0)).astype(BF16)

    def screens(put, begin, count, occ_parts, own, margin, bricks_y, lane_matrix, level):
        side = own // bricks_y
        cols = ROWS * len(occ_parts)
        shape = (own + 2 * margin if margin == 0 else own + ROWS, cols)
        brick = lax.div(iota(shape, 0) - margin + side, side) - 1
        place = jnp.where(
            brick < 0, ROWS + bricks_y - 1, jnp.where(brick >= bricks_y, 2 * ROWS, brick)
        )
        row_matrix = (place == iota(shape, 1)).astype(BF16)
        flags = [part[begin + x] for x in range(count) for part in occ_parts]
        wide = mm(jnp.concatenate(flags, axis=0).astype(BF16), lane_matrix).astype(BF16)
        for x in range(count):
            cells = mm(row_matrix, wide[x * cols : (x + 1) * cols])
            put(begin + x, weight[level] * (0.25 + cells))

    def chunked(ref):
        def put(j, value):
            for c in range(ref.shape[1]):
                ref[j, c] = value[:, c * LANES : (c + 1) * LANES]

        return put

    def put_coarse(j, value):
        cs[j] = value

    def coarse_view(begin, count):
        return cr.at[pl.ds(begin, count), rows_c]

    def mid_view(begin, count):
        return mb.at[pl.ds(begin, count), :, rows_m]

    near = slab_swap(coarse_view, xc, 1, 2)
    start(near)
    mid_flags = x_flags(om, bm[0]) + y_flags(om, om_l, om_r, bm[0])
    start(mid_flags)
    loads["w"].wait()
    screens(put_coarse, 1, bc[0], [oc], yc, 0, bc[1], lane_bricks(zc, bc[2], 1), 0)
    near_screens = [
        (copy(cs.at[bc[0]], cs.at[0], above), send_up, get_low),
        (copy(cs.at[1], cs.at[bc[0] + 1], below), send_down, get_high),
    ]
    start(near_screens)
    far = slab_swap(coarse_view, xc, 3, 2, 1, 2)
    start(far)

    loads["m"].wait()
    held = pl.ds(3 - 3 * iz, xm + 3)
    for c in range(cm):
        cols = slice(c * LANES, (c + 1) * LANES)
        block = in_m[pl.ds(iz * (xm - 3), xm + 3), :, cols].astype(F32)
        mb[pl.ds(PAD - 3 * iz, xm + 3), c, rows_m] = block
        m_up[held, c] = block[:, ym - 4 : ym]
        m_dn[held, c] = block[:, 0:4]
    mid_x = slab_swap(mid_view, xm, 3, 3)
    start(mid_x)
    mid_y = []
    for src, dst, step, can_send, can_recv in (
        (m_up, m_fu, 1, y_high, y_low), (m_dn, m_fd, -1, y_low, y_high)
    ):
        side = {"gy": iy + step}
        mid_y.append((copy(src.at[held], dst.at[held], side), can_send, can_recv))
        mid_y.append((copy(src.at[xm : xm + 3], dst.at[0:3], {**above, **side}),
                      both(can_send, send_up), both(can_recv, get_low)))
        mid_y.append((copy(src.at[3:6], dst.at[xm + 3 : xm + 6], {**below, **side}),
                      both(can_send, send_down), both(can_recv, get_high)))
    start(mid_y)

    loads["f"].wait()
    other = 1 - iz
    own_z, their_z = pl.ds(iz * ch, ch), pl.ds(other * ch, ch)

    def half_plane(p, c):
        return in_f[p, :, c * LANES : (c + 1) * LANES].astype(F32)

    def fill_fine(j, carry):
        for c in range(ch):
            zsend[j, c] = half_plane(other * (xf - 2) + j, c)
            fb[PAD - 2 * iz + j, iz * ch + c, rows_f] = half_plane(iz * (xf - 2) + j, c)
        return carry

    lax.fori_loop(0, xf + 2, fill_fine, 0, unroll=2)
    loads["of"].wait()
    own_flags = pl.ds(pl.multiple_of(iz * LANES, LANES), LANES)
    flags = jnp.concatenate(
        [io_f[...].astype(F32), jnp.zeros((bf[0], bf[1], LANES - bf[2]), F32)], axis=2
    )
    of[1 : 1 + bf[0], 0 : bf[1], own_flags] = flags
    partner = {"gz": other}
    z_fine = [
        (copy(zsend, fb.at[pl.ds(PAD - 2 * other, xf + 2), own_z, rows_f], partner), None, None),
        (copy(of.at[pl.ds(1, bf[0]), :, own_flags], of.at[pl.ds(1, bf[0]), :, own_flags], partner),
         None, None),
    ]
    start(z_fine[::-1])
    for c in range(ch):
        for k, p in enumerate((0, 1, nz * xf - 1)):
            edge[k, c] = half_plane(p, c)
    pair_up, made_up = copy(
        edge.at[pl.ds(2, 1)], fb.at[pl.ds(PAD - 1, 1), own_z, rows_f], above, iz, nz
    )
    pair_dn, made_dn = copy(
        edge.at[pl.ds(0, 2)], fb.at[pl.ds(PAD + xf, 2), own_z, rows_f], below, iz, nz
    )
    fine_x = [(pair_up, x_high, False), (pair_dn, x_low, False)]
    fine_x += [(c, False, get_low) for c in made_up] + [(c, False, get_high) for c in made_dn]
    start(fine_x)

    def wipe_rims(ref, own):
        shape = tuple(ref.shape)
        empty = jnp.zeros(shape[1:-2] + (TOP, LANES), F32)

        def one(p, carry):
            if len(shape) == 3:
                ref[p, 0:TOP] = empty
                ref[p, TOP + own :] = empty
            else:
                ref[p, :, 0:TOP] = empty
                ref[p, :, TOP + own :] = empty
            return carry

        lax.fori_loop(0, shape[0], one, 0)

    for ref in (cr, cw):
        wipe_rims(ref, yc)
    for ref in (mb, g1, g2, u1, u2, v0, v1, v2):
        wipe_rims(ref, ym)

    def z_lower(chunks):
        turned = [pltpu.roll(v, 1, 1) for v in chunks]
        edge_lane = iota(chunks[0].shape, 1) == 0
        return [
            jnp.where(edge_lane, turned[c - 1] if c else 0.0, turned[c])
            for c in range(len(chunks))
        ]

    def z_upper(chunks):
        turned = [pltpu.roll(v, LANES - 1, 1) for v in chunks]
        edge_lane = iota(chunks[0].shape, 1) == LANES - 1
        return [
            jnp.where(edge_lane, turned[c + 1] if c + 1 < len(chunks) else 0.0, turned[c])
            for c in range(len(chunks))
        ]

    def neighbours(load, chunks):
        low, high = z_lower(chunks), z_upper(chunks)
        return [
            (load(c, -1, 0) + load(c, 1, 0)) + (load(c, 0, -1) + load(c, 0, 1)) + (low[c] + high[c])
            for c in range(len(chunks))
        ]

    def later(load, chunks):
        high = z_upper(chunks)
        return [load(c, 1, 0) + load(c, 0, 1) + high[c] for c in range(len(chunks))]

    def view_of(ref, p, begin, count):
        def load(c, dx, dy):
            if len(ref.shape) == 3:
                return ref[p + dx, begin + dy : begin + dy + count]
            return ref[p + dx, c, begin + dy : begin + dy + count]

        return load, [load(c, 0, 0) for c in range(1 if len(ref.shape) == 3 else ref.shape[1])]

    def brick_of(own, side):
        return lambda p: lax.div(own * iz + p + (side - PAD), side)

    brick_c = brick_of(xc, nz * xc // bc[0])

    def coarse_w(p, carry):
        load, chunks = view_of(cr, p, TOP, yc)
        place = xc * slab + p - PAD
        keep = both(place >= 0, place < xc * slabs).astype(F32)
        cw[p, rows_c] = keep * (cs[brick_c(p)] * chunks[0] - neighbours(load, chunks)[0])
        return carry

    def coarse_moments(p, acc):
        load, chunks = view_of(cw, p, TOP, yc)
        r, w = cr[p, rows_c], chunks[0]
        image = cs[brick_c(p)] * w - 2.0 * later(load, chunks)[0]
        return tuple(a + fold_rows(b) for a, b in zip(acc, (r * r, r * w, w * w, w * image)))

    zero = jnp.zeros((ROWS, LANES), F32)
    lane_index = iota((1, LANES), 1)

    def spread_moments(values, buf, send, recv):
        row = jnp.zeros((1, LANES), F32)
        for k, a in values:
            value = jnp.sum(jnp.sum(a, axis=0, keepdims=True), axis=1, keepdims=True)
            row = jnp.where(lane_index == k, value, row)
        slot = (ix * ny + iy) * nz + iz
        buf[slot] = row
        copies = []
        for k, offset in enumerate(peers):
            c = pltpu.make_async_remote_copy(
                src_ref=buf.at[slot], dst_ref=buf.at[slot], send_sem=send.at[k],
                recv_sem=recv.at[k], device_id=at(offset), device_id_type=MESH,
            )
            c.start()
            copies.append(c)
        return copies

    def gathered(copies, buf):
        for c in copies:
            c.wait_recv()
        total = [buf[k] for k in range(buf.shape[0])]
        while len(total) > 1:
            total = [sum(total[k : k + 2][1:], total[k]) for k in range(0, len(total), 2)]
        return total[0]

    def picked(row, test):
        return jnp.sum(jnp.where(test, row, 0.0), axis=1, keepdims=True)

    def prolong(values, tz, put, lane_matrix, row_matrix):
        n, rows, lanes = values.shape
        high, low = split(values.reshape(n * rows, lanes))
        tz[...] = (mm(high, lane_matrix) + mm(low, lane_matrix)).reshape(tz.shape)
        twice = jnp.concatenate([row_matrix, row_matrix], axis=1)
        for j in range(n):
            put(j, mm(twice, jnp.concatenate(split(tz[j]), axis=0)))

    def interpolate(t, offset, count, g, own, begin, low, high, top):
        rows = t.shape[2]
        for p in range(PAD - low, PAD + own + high):
            m = p - PAD
            j = m // 2
            beside = min(max(j + (1 if m % 2 else -1) - begin, 0), count - 1)
            near_weight, side_weight = 0.75, 0.25
            if not 0 <= m < own:
                place = own * slab + m
                keep = both(place >= 0, place < own * slabs).astype(F32)
                near_weight, side_weight = 0.75 * keep, 0.25 * keep
            for c in range(t.shape[1]):
                g[p, c, top : top + rows] = (
                    near_weight * t[offset + j - begin, c] + side_weight * t[offset + beside, c]
                )

    def clear(ref, own, low, high):
        @pl.when(first)
        def _():
            wipe(ref, range(PAD - low, PAD))

        @pl.when(last)
        def _():
            wipe(ref, range(PAD + own, PAD + own + high))

    def row_masks(rows, margin, index, total):
        row = iota((rows + ROWS, LANES), 0) - margin + rows * index
        mask = both(row >= 0, row < total).astype(F32)
        return mask[0:ROWS], mask[rows:]

    def masked(v, masks):
        rows = v.shape[0] - ROWS
        return jnp.concatenate([v[0:ROWS] * masks[0], v[ROWS:rows], v[rows:] * masks[1]], axis=0)

    arrive(near)
    arrive(near_screens)
    relay_wait(0)
    relay_send(1)
    lax.fori_loop(PAD, PAD + xc + 1, coarse_w, 0, unroll=True)
    acc_c = lax.fori_loop(PAD, PAD + xc, coarse_moments, (zero,) * 4, unroll=True)
    mid_top = TOP - 4
    mid_lanes = lane_prolong(zm, zc)
    mid_rows = row_prolong(ym, 4, iy, ym * ny, yc, 0)
    arrive(mid_flags)
    screens(
        chunked(ms), 0, bm[0] + 2, [om, om_l, om_r], ym, 4, bm[1], lane_bricks(zm, bm[2], 1), 1
    )
    arrive(z_fine)
    fine_flags = x_flags(of, bf[0]) + y_flags(of, of_l, of_r, bf[0])
    start(fine_flags)
    arrive(far)
    lax.fori_loop(1, PAD, coarse_w, 0, unroll=True)
    lax.fori_loop(PAD + xc + 1, PAD + xc + 3, coarse_w, 0, unroll=True)
    count_c = xc + 6
    prolong(
        jnp.concatenate([cr[1 : 1 + count_c, rows_c], cw[1 : 1 + count_c, rows_c]], axis=0),
        ctz, chunked(ct), mid_lanes, mid_rows,
    )
    for k, ref in enumerate((g1, g2)):
        interpolate(ct, k * count_c, count_c, ref, xm, -3, 4, 4, mid_top)
    masks_m = row_masks(ym, 4, iy, ym * ny)
    brick_m = brick_of(xm, nz * xm // bm[0])
    window_m = slice(mid_top, mid_top + ym + ROWS)

    def mid_u(p, carry):
        brick = brick_m(p)
        for g, u in ((g1, u1), (g2, u2)):
            load, chunks = view_of(g, p, mid_top, ym + ROWS)
            for c, beside in enumerate(neighbours(load, chunks)):
                u[p, c, window_m] = masked((6.0 + ms[brick, c]) * chunks[c] - beside, masks_m)
        return carry

    lax.fori_loop(PAD - 3, PAD + xm + 3, mid_u, 0, unroll=True)
    for ref in (u1, u2):
        clear(ref, xm, 3, 3)
    arrive(mid_x)
    arrive(mid_y)
    for c in range(cm):
        mb[1 : xm + 7, c, TOP - 4 : TOP] = m_fu[:, c]
        mb[1 : xm + 7, c, TOP + ym : TOP + ym + 4] = m_fd[:, c]
    fields = ((mb, v0), (u1, v1), (u2, v2))

    def mid_v(p, carry):
        brick = brick_m(p)
        for u, v in fields:
            load, chunks = view_of(u, p, mid_top, ym + ROWS)
            for c, beside in enumerate(neighbours(load, chunks)):
                v[p, c, window_m] = masked(ms[brick, c] * chunks[c] - beside, masks_m)
        return carry

    lax.fori_loop(PAD - 2, PAD + xm + 2, mid_v, 0, unroll=True)
    for ref in (v0, v1, v2):
        clear(ref, xm, 2, 2)
    pairs_m = ((0, 0), (1, 1), (2, 2), (0, 1), (0, 2), (1, 2))

    def mid_moments(p, acc):
        brick = brick_m(p)
        views = [view_of(v, p, TOP, ym) for _, v in fields]
        beside = [later(load, chunks) for load, chunks in views]
        for c in range(cm):
            screen = ms[brick, c, 4 : 4 + ym]
            us = [u[p, c, rows_m] for u, _ in fields]
            vs = [chunks[c] for _, chunks in views]
            images = [screen * v - 2.0 * b[c] for v, b in zip(vs, beside)]
            values = [us[i] * us[j] for i, j in pairs_m] + [us[i] * vs[j] for i, j in pairs_m]
            values += [vs[i] * vs[j] for i, j in pairs_m]
            for i, j in pairs_m:
                cross = vs[i] * images[j]
                values.append(cross if i == j else 0.5 * (cross + vs[j] * images[i]))
            acc = tuple(a + fold_rows(v) for a, v in zip(acc, values))
        return acc

    acc = lax.fori_loop(PAD, PAD + xm, mid_moments, (zero,) * 24, unroll=2)
    relay_wait(1)
    for k in range(2, rounds):
        relay_send(k)
        relay_wait(k)
    slots = [(ROWS * (k // 6) + k % 6, a) for k, a in enumerate(acc)]
    slots += [(4 * ROWS + k, a) for k, a in enumerate(acc_c)]
    mid_copies = spread_moments(slots, am, sm, rm)

    arrive(fine_x)
    span = slice(PAD - 1, PAD + xf + 2)
    for c in range(cf):
        f_up[:, c] = fb[span, c, TOP + yf - 1 : TOP + yf]
        f_dn[:, c] = fb[span, c, TOP : TOP + 2]
    fine_y = [
        (copy(f_up, f_fu, {"gy": iy + 1}), y_high, y_low),
        (copy(f_dn, f_fd, {"gy": iy - 1}), y_low, y_high),
    ]
    start(fine_y)
    for ref in (fg, fr, fw):
        wipe_rims(ref, yf)
    fine_lanes = lane_prolong(zf, zm)
    fine_rows = row_prolong(yf, 2, iy, yf * ny, ym + ROWS, ym * iy - 4)
    masks_f = row_masks(yf, 2, iy, yf * ny)
    arrive(fine_flags)
    screens(
        chunked(fs), 0, bf[0] + 2, [of, of_l, of_r], yf, 2, bf[1], lane_bricks(zf, bf[2], nz), 2
    )
    arrive(fine_y)
    for c in range(cf):
        fb[span, c, TOP - 1 : TOP] = f_fu[:, c]
        fb[span, c, TOP + yf : TOP + yf + 2] = f_fd[:, c]
    total = gathered(mid_copies, am)
    ka, kb = coefficients(*[picked(total, lane_index == 4 * ROWS + k) for k in range(4)])
    weights = [None, ka * ka, kb * kb, -2.0 * ka, -2.0 * kb, 2.0 * ka * kb]
    kind = lane_index % ROWS
    scaled = total
    for k in range(1, 6):
        scaled = jnp.where(kind == k, total * weights[k], scaled)
    place = lax.div(lane_index, ROWS)
    km, kw = coefficients(*[
        picked(scaled, both(place == k, kind < 6)) for k in range(4)
    ])
    parts = (
        (g1, ka), (g2, kb), (mb, km), (u1, -km * ka), (u2, -km * kb),
        (v0, kw), (v1, -kw * ka), (v2, -kw * kb),
    )
    for p in range(2, xm + 6):
        for c in range(cm):
            value = parts[0][1] * parts[0][0][p, c, window_m]
            for ref, factor in parts[1:]:
                value = value + factor * ref[p, c, window_m]
            mx[p - 2, :, c * LANES : (c + 1) * LANES] = value
    own_c, own_m = pl.ds(iz * xc, xc), pl.ds(iz * xm, xm)

    prolong(mx[...], mtz, chunked(mt), fine_lanes, fine_rows)
    fine_top = TOP - 2
    interpolate(mt, 0, mt.shape[0], fg, xf, -2, 2, 3, fine_top)
    brick_f = brick_of(xf, nz * xf // bf[0])
    window_f = slice(fine_top, fine_top + yf + ROWS)

    def make_r(p, carry):
        brick = brick_f(p)
        load, chunks = view_of(fg, p, fine_top, yf + ROWS)
        for c, beside in enumerate(neighbours(load, chunks)):
            value = fb[p, c, window_f] - (6.0 + fs[brick, c]) * chunks[c] + beside
            fr[p, c, window_f] = masked(value, masks_f)
        return carry

    lax.fori_loop(PAD - 1, PAD + xf + 2, make_r, 0, unroll=UNROLL)
    clear(fr, xf, 1, 2)

    def make_w(p, carry):
        brick = brick_f(p)
        load, chunks = view_of(fr, p, fine_top, yf + ROWS)
        for c, beside in enumerate(neighbours(load, chunks)):
            fw[p, c, window_f] = masked(fs[brick, c] * chunks[c] - beside, masks_f)
        return carry

    lax.fori_loop(PAD, PAD + xf + 1, make_w, 0, unroll=UNROLL)
    clear(fw, xf, 0, 1)

    def moments(p, acc):
        brick = brick_f(p)
        load, chunks = view_of(fw, p, TOP, yf)
        for c, beside in enumerate(later(load, chunks)):
            r, w = fr[p, c, rows_f], chunks[c]
            image = fs[brick, c, 2 : 2 + yf] * w - 2.0 * beside
            acc = tuple(a + fold_rows(v) for a, v in zip(acc, (r * r, r * w, w * w, w * image)))
        return acc

    acc = lax.fori_loop(PAD, PAD + xf, moments, (zero,) * 4, unroll=UNROLL)
    fine_copies = spread_moments(list(enumerate(acc)), af, sf, rf)
    back = [
        (copy(src.at[PAD : PAD + xf, their_z, rows_f], dst, partner), None, None)
        for src, dst in ((fg, tg), (fr, tr), (fw, tw))
    ]
    start(back)
    out_c[own_c] = ka * cr[PAD : PAD + xc, rows_c] + kb * cw[PAD : PAD + xc, rows_c]
    out_m[own_m] = mx[2 : 2 + xm, 4 : 4 + ym, :]
    outs = [
        (copy(out_c.at[own_c], out_c.at[own_c], partner), None, None),
        (copy(out_m.at[own_m], out_m.at[own_m], partner), None, None),
    ]
    start(outs)
    for items in (
        near, near_screens, far, z_fine, mid_x, mid_flags, fine_x, mid_y, fine_flags, fine_y, outs
    ):
        left(items)
    for c in mid_copies:
        c.wait_send()
    arrive(outs)
    arrive(back)
    left(back)
    total = gathered(fine_copies, af)
    ka, kb = coefficients(*[picked(total, lane_index == k) for k in range(4)])
    coef[0] = jnp.broadcast_to(ka, (ROWS, LANES))
    coef[1] = jnp.broadcast_to(kb, (ROWS, LANES))
    for c in fine_copies:
        c.wait_send()


def finish(g, r, w, tg, tr, tw, coef, sol_c, sol_m, out_c, out_m, out_f, buf, sem):
    iz = lax.axis_index("gz")
    xs, ch, yf, _ = tg.shape
    small = [
        pltpu.make_async_copy(sol_c, out_c, sem.at[0]),
        pltpu.make_async_copy(sol_m, out_m, sem.at[1]),
    ]
    for c in small:
        c.start()
    ka, kb = coef[0, 0:1, 0:1], coef[1, 0:1, 0:1]
    rows = slice(TOP, TOP + yf)
    parts = 2
    step = xs // parts
    copies = list(small)
    for part in range(parts):
        for side in range(2):
            place = (iz if side == 0 else 1 - iz) * xs

            def one(x, carry):
                for c in range(ch):
                    if side == 0:
                        p, k = x + PAD, iz * ch + c
                        value = g[p, k, rows] + ka * r[p, k, rows] + kb * w[p, k, rows]
                    else:
                        value = tg[x, c] + ka * tr[x, c] + kb * tw[x, c]
                    buf[place + x, :, c * LANES : (c + 1) * LANES] = value
                return carry

            lax.fori_loop(part * step, part * step + step, one, 0, unroll=2)
            span = pl.ds(place + part * step, step)
            c = pltpu.make_async_copy(buf.at[span], out_f.at[span], sem.at[2 + 2 * part + side])
            c.start()
            copies.append(c)
    for c in copies:
        c.wait()


def shards(dims, *args):
    nx, ny, nz = dims
    rhs_c, rhs_m, rhs_f, occ_c, occ_m, occ_f, _ = args
    xc, yc, zc = rhs_c.shape
    xm, ym, zm = rhs_m.shape
    xf, yf, zh = rhs_f.shape
    zf = zh * nz
    xc, xm, xf = xc // nz, xm // nz, xf // nz
    cm, cf, ch = zm // LANES, zf // LANES, zh // LANES

    def buf(*shape):
        return pltpu.VMEM(shape, F32)

    def row(count, chunks, rows):
        return buf(count, chunks, rows, LANES)

    bm, bf = occ_m.shape[0] + 2, occ_f.shape[0] + 2
    scratch = [
        pltpu.VMEM(a.shape, a.dtype) for a in (rhs_c, rhs_m, rhs_f, occ_c, occ_m, occ_f)
    ]
    scratch += [pltpu.SMEM(args[6].shape, F32), pltpu.SemaphoreType.DMA((7,))]
    scratch += [
        buf(xc + 8, yc + 2 * TOP, zc), buf(xc + 8, yc + 2 * TOP, zc),
        buf(occ_c.shape[0] + 2, yc, zc),
        buf(2 * (xc + 6), yc, zm), row(2 * (xc + 6), cm, ym + ROWS),
        buf(occ_c.shape[0] + 2, ROWS, LANES),
    ]
    scratch += [row(xm + 8, cm, ym + 2 * TOP)] * 8
    scratch += [
        row(bm, cm, ym + ROWS),
        buf(xm + 4, ym + ROWS, zm), buf(xm + 4, ym + ROWS, zf), row(xm + 4, cf, yf + ROWS),
        buf(bm, ROWS, LANES),
        row(xm + 6, cm, 4), row(xm + 6, cm, 4), row(xm + 6, cm, 4), row(xm + 6, cm, 4),
        buf(bm, ROWS, LANES), buf(bm, ROWS, LANES),
        row(xf + 8, cf, yf + 2 * TOP), row(bf, cf, yf + ROWS), buf(bf, ROWS, nz * LANES),
        row(xf + 2, ch, yf), row(3, ch, yf),
        row(xf + 3, cf, 1), row(xf + 3, cf, 2), row(xf + 3, cf, 1), row(xf + 3, cf, 2),
        buf(bf, ROWS, nz * LANES), buf(bf, ROWS, nz * LANES),
        buf(nx * ny * nz, 1, LANES), buf(nx * ny * nz, 1, LANES),
    ]
    for count in (64, nx * ny * nz, nx * ny * nz):
        scratch += [pltpu.SemaphoreType.DMA((count,))] * 2
    scratch += [pltpu.SemaphoreType.REGULAR((max(nx, ny),))]
    hbm = pl.BlockSpec(memory_space=pltpu.HBM)
    vmem = pl.BlockSpec(memory_space=pltpu.VMEM)
    field = pltpu.VMEM((xf + 8, cf, yf + 2 * TOP, LANES), F32)
    half = pltpu.VMEM((xf, ch, yf, LANES), F32)
    made_shapes = [pltpu.VMEM(a.shape, F32) for a in args[:2]]
    made_shapes += [field] * 3 + [half] * 3 + [pltpu.VMEM((2, ROWS, LANES), F32)]
    room = sum(4 * math.prod(a.shape) for a in made_shapes)
    made = pl.pallas_call(
        functools.partial(kernel, dims),
        out_shape=made_shapes,
        in_specs=[hbm] * 7,
        out_specs=[vmem] * 9,
        scratch_shapes=scratch,
        compiler_params=pltpu.CompilerParams(
            collective_id=0, has_side_effects=True, vmem_limit_bytes=VMEM_BYTES - room
        ),
    )(*args)
    sol_c, sol_m, fields = made[0], made[1], made[2:]
    return pl.pallas_call(
        finish,
        out_shape=[jax.ShapeDtypeStruct(a.shape, F32) for a in args[:3]],
        in_specs=[vmem] * 9,
        out_specs=[hbm] * 3,
        scratch_shapes=[pltpu.VMEM(rhs_f.shape, F32), pltpu.SemaphoreType.DMA((6,))],
        compiler_params=pltpu.CompilerParams(vmem_limit_bytes=16 * 1024 * 1024),
    )(*fields, sol_c, sol_m)


def solution(mesh):
    dims = tuple(mesh.shape[axis] for axis in ("gx", "gy", "gz"))
    in_specs = (
        P("gx", None, None), P("gx", "gy", None), P("gx", "gy", "gz"),
        P("gx", None, None), P("gx", "gy", None), P("gx", "gy", "gz"), P(),
    )
    out_specs = (P("gx", None, None), P("gx", "gy", None), P("gx", "gy", "gz"))
    return jax.shard_map(
        functools.partial(shards, dims), mesh=mesh, in_specs=in_specs, out_specs=out_specs,
        check_vma=False,
    )
```

```python
import functools
import math

import jax
import jax.numpy as jnp
from jax import lax
from jax.experimental import pallas as pl
from jax.experimental.pallas import tpu as pltpu
from jax.sharding import PartitionSpec as P

MESH = pl.DeviceIdType.MESH
F32 = jnp.float32
BF16 = jnp.bfloat16
PAD = 4
ROWS = 8
TOP = 8
LANES = 128
VMEM_BYTES = 67043328


def iota(shape, dim):
    return lax.broadcasted_iota(jnp.int32, shape, dim)


def prolong_matrix(fine, coarse, total):
    base = lax.shift_right_arithmetic(fine, 1)
    beside = base + 2 * (fine & 1) - 1
    inside = jnp.logical_and(fine >= 0, fine < total)
    value = jnp.where(coarse == base, 0.75, jnp.where(coarse == beside, 0.25, 0.0))
    return jnp.where(inside, value, 0.0).astype(BF16)


def split(values):
    high = values.astype(BF16)
    return high, (values - high.astype(F32)).astype(BF16)


def mm(a, b):
    return jnp.dot(a, b, preferred_element_type=F32)


def fold_rows(values):
    total = values[0:ROWS]
    for row in range(ROWS, values.shape[0], ROWS):
        total = total + values[row : row + ROWS]
    out = total[:, 0:LANES]
    for lane in range(LANES, values.shape[1], LANES):
        out = out + total[:, lane : lane + LANES]
    return out


def coefficients(m0, n1, n2, n3):
    rho = n1 / m0
    spread = n2 - rho * n1
    bent = 6.0 * spread + (n3 - 2.0 * rho * n2 + rho * rho * n1)
    turn = jnp.where(bent > 0.0, jnp.maximum(spread, 0.0) / bent, 0.0)
    first = m0 / ((6.0 + rho) * m0 - jnp.maximum(spread, 0.0) * turn)
    second = -first * turn
    return first - second * rho, second


def kernel(
    dims,
    rhs_c, rhs_m, rhs_f, occ_c, occ_m, occ_f, weight_in,
    out_c, out_m, fg, fr, fw, tg, tr, tw, coef,
    in_c, in_m, in_f, io_c, io_m, io_f, weight, isem,
    cr, cw, cs, ctz, ct, oc,
    mb, g1, g2, u1, u2, v0, v1, v2, ms, mx, mtz, mt, om, m_up, m_dn, m_fu, m_fd, om_l, om_r,
    fb, fs, of, zsend, edge, f_up, f_dn, f_fu, f_fd, of_l, of_r,
    am, af, ss, rs, sm, rm, sf, rf, relay,
):
    nx, ny, nz = dims
    ix, iy, iz = lax.axis_index("gx"), lax.axis_index("gy"), lax.axis_index("gz")
    xc, yc, zc = rhs_c.shape
    xm, ym, zm = rhs_m.shape
    xf, yf, zh = rhs_f.shape
    zf = zh * nz
    xc, xm, xf = xc // nz, xm // nz, xf // nz
    cm, cf, ch = zm // LANES, zf // LANES, zh // LANES
    slab = ix * nz + iz
    slabs = nx * nz
    bc, bm, bf = occ_c.shape, occ_m.shape, occ_f.shape
    x_low, x_high = ix > 0, ix < nx - 1
    y_low, y_high = iy > 0, iy < ny - 1
    lower, upper = iz == 0, iz == 1
    first, last = slab == 0, slab == slabs - 1
    rows_c, rows_m, rows_f = (slice(TOP, TOP + n) for n in (yc, ym, yf))

    def both(a, b):
        return jnp.logical_and(a, b)

    def at(offset):
        return (
            lax.rem(ix + offset[0], nx), lax.rem(iy + offset[1], ny), lax.rem(iz + offset[2], nz)
        )

    loads = {}
    pairs = (
        ("c", rhs_c, in_c), ("oc", occ_c, io_c), ("om", occ_m, io_m), ("w", weight_in, weight),
        ("m", rhs_m, in_m), ("f", rhs_f, in_f), ("of", occ_f, io_f),
    )
    for k, (name, src, dst) in enumerate(pairs):
        loads[name] = pltpu.make_async_copy(src, dst, isem.at[k])
        loads[name].start()

    for ref in (oc, om, of, om_l, om_r, of_l, of_r):
        ref[...] = jnp.zeros_like(ref)

    barrier = pltpu.get_barrier_semaphore()
    peers = [(a, b, c) for a in range(nx) for b in range(ny) for c in range(nz)][1:]
    around = [(a, b) for a in (-1, 1, 0) for b in (-1, 1, 0)]

    def greet(semaphore, a, b, c):
        def send():
            pl.semaphore_signal(
                semaphore, inc=1, device_id=(ix + a, iy + b, c), device_id_type=MESH
            )

        tests = ((x_low, a < 0), (x_high, a > 0), (y_low, b < 0), (y_high, b > 0))
        there = [test for test, needed in tests if needed]
        if there:
            pl.when(functools.reduce(both, there))(send)
        else:
            send()

    for a, b in around:
        for c in range(1 if (a, b) == (0, 0) else 0, nz):
            greet(barrier, a, b, lax.rem(iz + c, nz))
    chips = (1 + jnp.where(x_low, 1, 0) + jnp.where(x_high, 1, 0)) * (
        1 + jnp.where(y_low, 1, 0) + jnp.where(y_high, 1, 0)
    )
    rounds = max(nx, ny) - 2

    def relay_send(k):
        if k < rounds:
            for a, b in around[:-1]:
                greet(relay.at[k], a, b, iz)

    def relay_wait(k):
        if k < rounds:
            pl.semaphore_wait(relay.at[k], chips - 1)

    def wipe(ref, planes):
        for p in planes:
            ref[p] = jnp.zeros(tuple(ref.shape[1:]), F32)

    @pl.when(first)
    def _():
        wipe(cr, range(0, 4))
        wipe(cs, (0,))
        wipe(mb, range(1, 4))
        wipe(fb, range(2, 4))
        for ref in (m_fu, m_fd):
            wipe(ref, range(0, 3))

    @pl.when(last)
    def _():
        wipe(cr, range(PAD + xc, PAD + xc + 4))
        wipe(cs, (bc[0] + 1,))
        wipe(mb, range(PAD + xm, PAD + xm + 3))
        wipe(fb, range(PAD + xf, PAD + xf + 2))
        for ref in (m_fu, m_fd):
            wipe(ref, range(xm + 3, xm + 6))

    @pl.when(jnp.logical_not(x_low))
    def _():
        for ref in (om_l, om_r, of_l, of_r):
            wipe(ref, (0,))

    @pl.when(jnp.logical_not(x_high))
    def _():
        for ref in (om_l, om_r, of_l, of_r):
            wipe(ref, (ref.shape[0] - 1,))

    @pl.when(jnp.logical_not(y_low))
    def _():
        for ref in (m_fu, f_fu, om_l, of_l):
            ref[...] = jnp.zeros_like(ref)

    @pl.when(jnp.logical_not(y_high))
    def _():
        for ref in (m_fd, f_fd, om_r, of_r):
            ref[...] = jnp.zeros_like(ref)

    loads["oc"].wait()
    oc[1 : 1 + bc[0], 0 : bc[1], 0 : bc[2]] = io_c[...].astype(F32)
    loads["om"].wait()
    om[1 : 1 + bm[0], 0 : bm[1], 0 : bm[2]] = io_m[...].astype(F32)
    loads["c"].wait()
    cr[pl.ds(PAD - 4 * iz, xc + 4), rows_c] = in_c[pl.ds(iz * (xc - 4), xc + 4)].astype(F32)

    def row_prolong(own, margin, index, total, cols, col_first):
        shape = (own + ROWS, cols)
        fine = iota(shape, 0) - margin + own * index
        return prolong_matrix(fine, iota(shape, 1) + col_first, total)

    def lane_prolong(cells, rows):
        shape = (rows, cells)
        return prolong_matrix(iota(shape, 1), iota(shape, 0), cells)

    def lane_bricks(cells, bricks, halves):
        shape = (halves * LANES, cells)
        brick = lax.div(iota(shape, 1), cells // (bricks * halves))
        place = brick + lax.div(brick, bricks) * (LANES - bricks)
        return (place == iota(shape, 0)).astype(BF16)

    def screens(put, begin, count, occ_parts, own, margin, bricks_y, lane_matrix, level):
        side = own // bricks_y
        cols = ROWS * len(occ_parts)
        shape = (own + 2 * margin if margin == 0 else own + ROWS, cols)
        brick = lax.div(iota(shape, 0) - margin + side, side) - 1
        place = jnp.where(
            brick < 0, ROWS + bricks_y - 1, jnp.where(brick >= bricks_y, 2 * ROWS, brick)
        )
        row_matrix = (place == iota(shape, 1)).astype(BF16)
        flags = [part[begin + x] for x in range(count) for part in occ_parts]
        wide = mm(jnp.concatenate(flags, axis=0).astype(BF16), lane_matrix).astype(BF16)
        for x in range(count):
            cells = mm(row_matrix, wide[x * cols : (x + 1) * cols])
            put(begin + x, weight[level] * (0.25 + cells))

    def chunked(ref):
        def put(j, value):
            for c in range(ref.shape[1]):
                ref[j, c] = value[:, c * LANES : (c + 1) * LANES]

        return put

    def put_coarse(j, value):
        cs[j] = value

    loads["w"].wait()
    screens(put_coarse, 1, bc[0], [oc], yc, 0, bc[1], lane_bricks(zc, bc[2], 1), 0)
    loads["m"].wait()
    held = pl.ds(3 - 3 * iz, xm + 3)
    for c in range(cm):
        cols = slice(c * LANES, (c + 1) * LANES)
        block = in_m[pl.ds(iz * (xm - 3), xm + 3), :, cols].astype(F32)
        mb[pl.ds(PAD - 3 * iz, xm + 3), c, rows_m] = block
        m_up[held, c] = block[:, ym - 4 : ym]
        m_dn[held, c] = block[:, 0:4]
    pl.semaphore_wait(barrier, chips * nz - 1)
    relay_send(0)

    used = [0]

    def copy(src, dst, target, step=0, count=1):
        k = used[0]
        used[0] += count

        def made(j):
            return pltpu.make_async_remote_copy(
                src_ref=src, dst_ref=dst, send_sem=ss.at[k], recv_sem=rs.at[k + j],
                device_id=target, device_id_type=MESH,
            )

        return made(0) if count == 1 else (made(step), [made(j) for j in range(count)])

    def start(items):
        for c, can_send, _ in items:
            if can_send is None:
                c.start()
            elif can_send is not False:
                pl.when(can_send)(c.start)

    def arrive(items):
        for c, _, can_recv in items:
            if can_recv is None:
                c.wait_recv()
            elif can_recv is not False:
                pl.when(can_recv)(c.wait_recv)

    def left(items):
        for c, can_send, _ in items:
            if can_send is None:
                c.wait_send()
            elif can_send is not False:
                pl.when(can_send)(c.wait_send)

    above, below = {"gx": ix + 1, "gz": 0}, {"gx": ix - 1, "gz": 1}
    send_up, get_low = both(upper, x_high), both(lower, x_low)
    send_down, get_high = both(lower, x_low), both(upper, x_high)

    def slab_swap(view, own, width_low, width_high, skip_low=0, skip_high=0):
        stop, begin = PAD + own - skip_low, PAD + skip_high
        low = PAD - skip_low - width_low
        return [
            (copy(view(stop - width_low, width_low), view(low, width_low), above),
             send_up, get_low),
            (copy(view(begin, width_high), view(begin + own, width_high), below),
             send_down, get_high),
        ]

    def brick_rows(bricks):
        return slice(0, bricks[1])

    def x_flags(occ, bricks, rows):
        return [
            (copy(occ.at[bricks, rows], occ.at[0, rows], {"gx": ix + 1}), x_high, x_low),
            (copy(occ.at[1, rows], occ.at[bricks + 1, rows], {"gx": ix - 1}), x_low, x_high),
        ]

    def y_flags(occ, occ_l, occ_r, bricks, rows):
        items = []
        flags = pl.ds(1, bricks)
        for dst, step, can_send, can_recv in (
            (occ_l, 1, y_high, y_low), (occ_r, -1, y_low, y_high)
        ):
            items.append((copy(occ.at[flags, rows], dst.at[flags, rows], {"gy": iy + step}), can_send, can_recv))
            items.append((copy(occ.at[bricks, rows], dst.at[0, rows], {"gx": ix + 1, "gy": iy + step}),
                          both(can_send, x_high), both(can_recv, x_low)))
            items.append((copy(occ.at[1, rows], dst.at[bricks + 1, rows], {"gx": ix - 1, "gy": iy + step}),
                          both(can_send, x_low), both(can_recv, x_high)))
        return items

    def coarse_view(begin, count):
        return cr.at[pl.ds(begin, count), rows_c]

    def mid_view(begin, count):
        return mb.at[pl.ds(begin, count), :, rows_m]

    near = slab_swap(coarse_view, xc, 1, 2)
    start(near)
    mid_flags = x_flags(om, bm[0], brick_rows(bm)) + y_flags(om, om_l, om_r, bm[0], brick_rows(bm))
    start(mid_flags)
    near_screens = [
        (copy(cs.at[bc[0]], cs.at[0], above), send_up, get_low),
        (copy(cs.at[1], cs.at[bc[0] + 1], below), send_down, get_high),
    ]
    start(near_screens)
    far = slab_swap(coarse_view, xc, 3, 2, 1, 2)
    start(far)

    mid_x = slab_swap(mid_view, xm, 3, 3)
    start(mid_x)
    mid_y = []
    for src, dst, step, can_send, can_recv in (
        (m_up, m_fu, 1, y_high, y_low), (m_dn, m_fd, -1, y_low, y_high)
    ):
        side = {"gy": iy + step}
        mid_y.append((copy(src.at[held], dst.at[held], side), can_send, can_recv))
        mid_y.append((copy(src.at[xm : xm + 3], dst.at[0:3], {**above, **side}),
                      both(can_send, send_up), both(can_recv, get_low)))
        mid_y.append((copy(src.at[3:6], dst.at[xm + 3 : xm + 6], {**below, **side}),
                      both(can_send, send_down), both(can_recv, get_high)))
    start(mid_y)

    loads["f"].wait()
    other = 1 - iz
    own_z, their_z = pl.ds(iz * ch, ch), pl.ds(other * ch, ch)

    def half_plane(p, c):
        return in_f[p, :, c * LANES : (c + 1) * LANES].astype(F32)

    def fill_fine(j, carry):
        for c in range(ch):
            zsend[j, c] = half_plane(other * (xf - 2) + j, c)
            fb[PAD - 2 * iz + j, iz * ch + c, rows_f] = half_plane(iz * (xf - 2) + j, c)
        return carry

    lax.fori_loop(0, xf + 2, fill_fine, 0, unroll=2)
    loads["of"].wait()
    own_flags = pl.ds(pl.multiple_of(iz * LANES, LANES), LANES)
    flags = jnp.concatenate(
        [io_f[...].astype(F32), jnp.zeros((bf[0], bf[1], LANES - bf[2]), F32)], axis=2
    )
    of[1 : 1 + bf[0], 0 : bf[1], own_flags] = flags
    partner = {"gz": other}
    z_fine = [
        (copy(zsend, fb.at[pl.ds(PAD - 2 * other, xf + 2), own_z, rows_f], partner), None, None),
        (copy(of.at[pl.ds(1, bf[0]), :, own_flags], of.at[pl.ds(1, bf[0]), :, own_flags], partner),
         None, None),
    ]
    start(z_fine[::-1])
    def wipe_rims(ref, own):
        shape = tuple(ref.shape)
        empty = jnp.zeros(shape[1:-2] + (TOP, LANES), F32)

        def one(p, carry):
            if len(shape) == 3:
                ref[p, 0:TOP] = empty
                ref[p, TOP + own :] = empty
            else:
                ref[p, :, 0:TOP] = empty
                ref[p, :, TOP + own :] = empty
            return carry

        lax.fori_loop(0, shape[0], one, 0)

    for ref in (cr, cw):
        wipe_rims(ref, yc)
    for ref in (mb, g1, g2, u1, u2, v0, v1, v2):
        wipe_rims(ref, ym)

    def z_lower(chunks):
        turned = [pltpu.roll(v, 1, 1) for v in chunks]
        edge_lane = iota(chunks[0].shape, 1) == 0
        return [
            jnp.where(edge_lane, turned[c - 1] if c else 0.0, turned[c])
            for c in range(len(chunks))
        ]

    def z_upper(chunks):
        turned = [pltpu.roll(v, LANES - 1, 1) for v in chunks]
        edge_lane = iota(chunks[0].shape, 1) == LANES - 1
        return [
            jnp.where(edge_lane, turned[c + 1] if c + 1 < len(chunks) else 0.0, turned[c])
            for c in range(len(chunks))
        ]

    def neighbours(load, chunks):
        low, high = z_lower(chunks), z_upper(chunks)
        return [
            (load(c, -1, 0) + load(c, 1, 0)) + (load(c, 0, -1) + load(c, 0, 1)) + (low[c] + high[c])
            for c in range(len(chunks))
        ]

    def later(load, chunks):
        high = z_upper(chunks)
        return [load(c, 1, 0) + load(c, 0, 1) + high[c] for c in range(len(chunks))]

    def view_of(ref, p, begin, count):
        def load(c, dx, dy):
            if len(ref.shape) == 3:
                return ref[p + dx, begin + dy : begin + dy + count]
            return ref[p + dx, c, begin + dy : begin + dy + count]

        return load, [load(c, 0, 0) for c in range(1 if len(ref.shape) == 3 else ref.shape[1])]

    def brick_of(own, side):
        return lambda p: lax.div(own * iz + p + (side - PAD), side)

    brick_c = brick_of(xc, nz * xc // bc[0])

    def coarse_w(p, carry):
        load, chunks = view_of(cr, p, TOP, yc)
        place = xc * slab + p - PAD
        keep = both(place >= 0, place < xc * slabs).astype(F32)
        cw[p, rows_c] = keep * (cs[brick_c(p)] * chunks[0] - neighbours(load, chunks)[0])
        return carry

    def coarse_moments(p, acc):
        load, chunks = view_of(cw, p, TOP, yc)
        r, w = cr[p, rows_c], chunks[0]
        image = cs[brick_c(p)] * w - 2.0 * later(load, chunks)[0]
        return tuple(a + fold_rows(b) for a, b in zip(acc, (r * r, r * w, w * w, w * image)))

    zero = jnp.zeros((ROWS, LANES), F32)
    lane_index = iota((1, LANES), 1)

    def spread_moments(values, buf, send, recv):
        row = jnp.zeros((1, LANES), F32)
        for k, a in values:
            value = jnp.sum(jnp.sum(a, axis=0, keepdims=True), axis=1, keepdims=True)
            row = jnp.where(lane_index == k, value, row)
        slot = (ix * ny + iy) * nz + iz
        buf[slot] = row
        copies = []
        for k, offset in enumerate(peers):
            c = pltpu.make_async_remote_copy(
                src_ref=buf.at[slot], dst_ref=buf.at[slot], send_sem=send.at[k],
                recv_sem=recv.at[k], device_id=at(offset), device_id_type=MESH,
            )
            c.start()
            copies.append(c)
        return copies

    def gathered(copies, buf):
        for c in copies:
            c.wait_recv()
        total = [buf[k] for k in range(buf.shape[0])]
        while len(total) > 1:
            total = [sum(total[k : k + 2][1:], total[k]) for k in range(0, len(total), 2)]
        return total[0]

    def picked(row, test):
        return jnp.sum(jnp.where(test, row, 0.0), axis=1, keepdims=True)

    def prolong(values, tz, put, lane_matrix, row_matrix):
        n, rows, lanes = values.shape
        high, low = split(values.reshape(n * rows, lanes))
        tz[...] = (mm(high, lane_matrix) + mm(low, lane_matrix)).reshape(tz.shape)
        twice = jnp.concatenate([row_matrix, row_matrix], axis=1)
        for j in range(n):
            put(j, mm(twice, jnp.concatenate(split(tz[j]), axis=0)))

    def interpolate(t, offset, count, g, own, begin, low, high, top):
        rows = t.shape[2]
        for p in range(PAD - low, PAD + own + high):
            m = p - PAD
            j = m // 2
            beside = min(max(j + (1 if m % 2 else -1) - begin, 0), count - 1)
            near_weight, side_weight = 0.75, 0.25
            if not 0 <= m < own:
                place = own * slab + m
                keep = both(place >= 0, place < own * slabs).astype(F32)
                near_weight, side_weight = 0.75 * keep, 0.25 * keep
            for c in range(t.shape[1]):
                g[p, c, top : top + rows] = (
                    near_weight * t[offset + j - begin, c] + side_weight * t[offset + beside, c]
                )

    def clear(ref, own, low, high):
        @pl.when(first)
        def _():
            wipe(ref, range(PAD - low, PAD))

        @pl.when(last)
        def _():
            wipe(ref, range(PAD + own, PAD + own + high))

    def row_masks(rows, margin, index, total):
        row = iota((rows + ROWS, LANES), 0) - margin + rows * index
        mask = both(row >= 0, row < total).astype(F32)
        return mask[0:ROWS], mask[rows:]

    def masked(v, masks):
        rows = v.shape[0] - ROWS
        return jnp.concatenate([v[0:ROWS] * masks[0], v[ROWS:rows], v[rows:] * masks[1]], axis=0)

    relay_wait(0)
    relay_send(1)
    for c in range(ch):
        for k, p in enumerate((0, 1, nz * xf - 1)):
            edge[k, c] = half_plane(p, c)
    pair_up, made_up = copy(
        edge.at[pl.ds(2, 1)], fb.at[pl.ds(PAD - 1, 1), own_z, rows_f], above, iz, nz
    )
    pair_dn, made_dn = copy(
        edge.at[pl.ds(0, 2)], fb.at[pl.ds(PAD + xf, 2), own_z, rows_f], below, iz, nz
    )
    fine_x = [(pair_up, x_high, False), (pair_dn, x_low, False)]
    fine_x += [(c, False, get_low) for c in made_up] + [(c, False, get_high) for c in made_dn]
    start(fine_x)

    arrive(near)
    arrive(near_screens)
    lax.fori_loop(PAD, PAD + xc + 1, coarse_w, 0, unroll=True)
    acc_c = lax.fori_loop(PAD, PAD + xc, coarse_moments, (zero,) * 4, unroll=True)
    mid_top = TOP - 4
    mid_lanes = lane_prolong(zm, zc)
    mid_rows = row_prolong(ym, 4, iy, ym * ny, yc, 0)
    arrive(z_fine)
    fine_flags = x_flags(of, bf[0], brick_rows(bf)) + y_flags(of, of_l, of_r, bf[0], brick_rows(bf))
    start(fine_flags)
    arrive(far)
    lax.fori_loop(1, PAD, coarse_w, 0, unroll=True)
    lax.fori_loop(PAD + xc + 1, PAD + xc + 3, coarse_w, 0, unroll=True)
    count_c = xc + 6
    twice_m = jnp.concatenate([mid_rows, mid_rows], axis=1)
    for j in range(count_c):
        planes = jnp.concatenate([cr[1 + j, rows_c], cw[1 + j, rows_c]], axis=1)
        made_rows = mm(twice_m, jnp.concatenate(split(planes), axis=0))
        ctz[j] = made_rows[:, 0:zc]
        ctz[count_c + j] = made_rows[:, zc:]
    high, low = split(ctz[...].reshape(2 * count_c * (ym + ROWS), zc))
    spread_z = mm(high, mid_lanes) + mm(low, mid_lanes)
    for c in range(cm):
        ct[:, c] = spread_z[:, c * LANES : (c + 1) * LANES].reshape(
            2 * count_c, ym + ROWS, LANES
        )
    for k, ref in enumerate((g1, g2)):
        interpolate(ct, k * count_c, count_c, ref, xm, -3, 4, 4, mid_top)
    arrive(mid_flags)
    screens(
        chunked(ms), 0, bm[0] + 2, [om, om_l, om_r], ym, 4, bm[1], lane_bricks(zm, bm[2], 1), 1
    )
    masks_m = row_masks(ym, 4, iy, ym * ny)
    brick_m = brick_of(xm, nz * xm // bm[0])
    window_m = slice(mid_top, mid_top + ym + ROWS)

    def mid_u(p, carry):
        brick = brick_m(p)
        for g, u in ((g1, u1), (g2, u2)):
            load, chunks = view_of(g, p, mid_top, ym + ROWS)
            for c, beside in enumerate(neighbours(load, chunks)):
                u[p, c, window_m] = masked((6.0 + ms[brick, c]) * chunks[c] - beside, masks_m)
        return carry

    lax.fori_loop(PAD - 3, PAD + xm + 3, mid_u, 0, unroll=True)
    for ref in (u1, u2):
        clear(ref, xm, 3, 3)
    arrive(mid_x)
    arrive(mid_y)
    for c in range(cm):
        mb[1 : xm + 7, c, TOP - 4 : TOP] = m_fu[:, c]
        mb[1 : xm + 7, c, TOP + ym : TOP + ym + 4] = m_fd[:, c]
    fields = ((mb, v0), (u1, v1), (u2, v2))

    def mid_v(p, carry):
        brick = brick_m(p)
        for u, v in fields:
            load, chunks = view_of(u, p, mid_top, ym + ROWS)
            for c, beside in enumerate(neighbours(load, chunks)):
                v[p, c, window_m] = masked(ms[brick, c] * chunks[c] - beside, masks_m)
        return carry

    lax.fori_loop(PAD - 2, PAD + xm + 2, mid_v, 0, unroll=True)
    for ref in (v0, v1, v2):
        clear(ref, xm, 2, 2)
    pairs_m = ((0, 0), (1, 1), (2, 2), (0, 1), (0, 2), (1, 2))

    def mid_moments(p, acc):
        brick = brick_m(p)
        views = [view_of(v, p, TOP, ym) for _, v in fields]
        beside = [later(load, chunks) for load, chunks in views]
        for c in range(cm):
            screen = ms[brick, c, 4 : 4 + ym]
            us = [u[p, c, rows_m] for u, _ in fields]
            vs = [chunks[c] for _, chunks in views]
            images = [screen * v - 2.0 * b[c] for v, b in zip(vs, beside)]
            values = [us[i] * us[j] for i, j in pairs_m] + [us[i] * vs[j] for i, j in pairs_m]
            values += [vs[i] * vs[j] for i, j in pairs_m]
            for i, j in pairs_m:
                cross = vs[i] * images[j]
                values.append(cross if i == j else 0.5 * (cross + vs[j] * images[i]))
            acc = tuple(a + fold_rows(v) for a, v in zip(acc, values))
        return acc

    acc = lax.fori_loop(PAD, PAD + xm, mid_moments, (zero,) * 24, unroll=2)
    relay_wait(1)
    for k in range(2, rounds):
        relay_send(k)
        relay_wait(k)
    slots = [(ROWS * (k // 6) + k % 6, a) for k, a in enumerate(acc)]
    slots += [(4 * ROWS + k, a) for k, a in enumerate(acc_c)]
    mid_copies = spread_moments(slots, am, sm, rm)

    arrive(fine_x)
    span = slice(PAD - 1, PAD + xf + 2)
    for c in range(cf):
        f_up[:, c] = fb[span, c, TOP + yf - 1 : TOP + yf]
        f_dn[:, c] = fb[span, c, TOP : TOP + 2]
    fine_y = [
        (copy(f_up, f_fu, {"gy": iy + 1}), y_high, y_low),
        (copy(f_dn, f_fd, {"gy": iy - 1}), y_low, y_high),
    ]
    start(fine_y)
    for ref in (fg, fr, fw):
        wipe_rims(ref, yf)
    fine_lanes = lane_prolong(zf, zm)
    fine_rows = row_prolong(yf, 2, iy, yf * ny, ym + ROWS, ym * iy - 4)
    masks_f = row_masks(yf, 2, iy, yf * ny)
    arrive(fine_flags)
    screens(
        chunked(fs), 0, bf[0] + 2, [of, of_l, of_r], yf, 2, bf[1], lane_bricks(zf, bf[2], nz), 2
    )
    arrive(fine_y)
    for c in range(cf):
        fb[span, c, TOP - 1 : TOP] = f_fu[:, c]
        fb[span, c, TOP + yf : TOP + yf + 2] = f_fd[:, c]
    total = gathered(mid_copies, am)
    ka, kb = coefficients(*[picked(total, lane_index == 4 * ROWS + k) for k in range(4)])
    weights = [None, ka * ka, kb * kb, -2.0 * ka, -2.0 * kb, 2.0 * ka * kb]
    kind = lane_index % ROWS
    scaled = total
    for k in range(1, 6):
        scaled = jnp.where(kind == k, total * weights[k], scaled)
    place = lax.div(lane_index, ROWS)
    km, kw = coefficients(*[
        picked(scaled, both(place == k, kind < 6)) for k in range(4)
    ])
    parts = (
        (g1, ka), (g2, kb), (mb, km), (u1, -km * ka), (u2, -km * kb),
        (v0, kw), (v1, -kw * ka), (v2, -kw * kb),
    )
    for p in range(2, xm + 6):
        for c in range(cm):
            value = parts[0][1] * parts[0][0][p, c, window_m]
            for ref, factor in parts[1:]:
                value = value + factor * ref[p, c, window_m]
            mx[p - 2, :, c * LANES : (c + 1) * LANES] = value
    own_c, own_m = pl.ds(iz * xc, xc), pl.ds(iz * xm, xm)

    prolong(mx[...], mtz, chunked(mt), fine_lanes, fine_rows)
    fine_top = TOP - 2
    interpolate(mt, 0, mt.shape[0], fg, xf, -2, 2, 3, fine_top)
    brick_f = brick_of(xf, nz * xf // bf[0])
    window_f = slice(fine_top, fine_top + yf + ROWS)

    def make_r(p, carry):
        brick = brick_f(p)
        load, chunks = view_of(fg, p, fine_top, yf + ROWS)
        for c, beside in enumerate(neighbours(load, chunks)):
            value = fb[p, c, window_f] - (6.0 + fs[brick, c]) * chunks[c] + beside
            fr[p, c, window_f] = masked(value, masks_f)
        return carry

    lax.fori_loop(PAD - 1, PAD + xf + 2, make_r, 0, unroll=True)
    clear(fr, xf, 1, 2)

    def make_w(p, carry):
        brick = brick_f(p)
        load, chunks = view_of(fr, p, fine_top, yf + ROWS)
        for c, beside in enumerate(neighbours(load, chunks)):
            fw[p, c, window_f] = masked(fs[brick, c] * chunks[c] - beside, masks_f)
        return carry

    lax.fori_loop(PAD, PAD + xf + 1, make_w, 0, unroll=True)
    clear(fw, xf, 0, 1)

    def moments(p, acc):
        brick = brick_f(p)
        load, chunks = view_of(fw, p, TOP, yf)
        for c, beside in enumerate(later(load, chunks)):
            r, w = fr[p, c, rows_f], chunks[c]
            image = fs[brick, c, 2 : 2 + yf] * w - 2.0 * beside
            acc = tuple(a + fold_rows(v) for a, v in zip(acc, (r * r, r * w, w * w, w * image)))
        return acc

    acc = lax.fori_loop(PAD, PAD + xf, moments, (zero,) * 4, unroll=True)
    fine_copies = spread_moments(list(enumerate(acc)), af, sf, rf)
    back = [
        (copy(src.at[PAD : PAD + xf, their_z, rows_f], dst, partner), None, None)
        for src, dst in ((fg, tg), (fr, tr), (fw, tw))
    ]
    start(back)
    out_c[own_c] = ka * cr[PAD : PAD + xc, rows_c] + kb * cw[PAD : PAD + xc, rows_c]
    out_m[own_m] = mx[2 : 2 + xm, 4 : 4 + ym, :]
    outs = [
        (copy(out_c.at[own_c], out_c.at[own_c], partner), None, None),
        (copy(out_m.at[own_m], out_m.at[own_m], partner), None, None),
    ]
    start(outs)
    for items in (
        near, near_screens, far, z_fine, mid_x, mid_flags, fine_x, mid_y, fine_flags, fine_y, outs
    ):
        left(items)
    for c in mid_copies:
        c.wait_send()
    arrive(outs)
    arrive(back)
    left(back)
    total = gathered(fine_copies, af)
    ka, kb = coefficients(*[picked(total, lane_index == k) for k in range(4)])
    coef[0] = jnp.broadcast_to(ka, (ROWS, LANES))
    coef[1] = jnp.broadcast_to(kb, (ROWS, LANES))
    for c in fine_copies:
        c.wait_send()


def finish(g, r, w, tg, tr, tw, coef, sol_c, sol_m, out_c, out_m, out_f, buf, sem):
    iz = lax.axis_index("gz")
    xs, ch, yf, _ = tg.shape
    small = [
        pltpu.make_async_copy(sol_c, out_c, sem.at[0]),
        pltpu.make_async_copy(sol_m, out_m, sem.at[1]),
    ]
    for c in small:
        c.start()
    ka, kb = coef[0, 0:1, 0:1], coef[1, 0:1, 0:1]
    rows = slice(TOP, TOP + yf)
    parts = 2
    step = xs // parts
    copies = list(small)
    for part in range(parts):
        for side in range(2):
            place = (iz if side == 0 else 1 - iz) * xs

            def one(x, carry):
                for c in range(ch):
                    if side == 0:
                        p, k = x + PAD, iz * ch + c
                        value = g[p, k, rows] + ka * r[p, k, rows] + kb * w[p, k, rows]
                    else:
                        value = tg[x, c] + ka * tr[x, c] + kb * tw[x, c]
                    buf[place + x, :, c * LANES : (c + 1) * LANES] = value
                return carry

            lax.fori_loop(part * step, part * step + step, one, 0, unroll=True)
            span = pl.ds(place + part * step, step)
            c = pltpu.make_async_copy(buf.at[span], out_f.at[span], sem.at[2 + 2 * part + side])
            c.start()
            copies.append(c)
    for c in copies:
        c.wait()


def shards(dims, *args):
    nx, ny, nz = dims
    rhs_c, rhs_m, rhs_f, occ_c, occ_m, occ_f, _ = args
    xc, yc, zc = rhs_c.shape
    xm, ym, zm = rhs_m.shape
    xf, yf, zh = rhs_f.shape
    zf = zh * nz
    xc, xm, xf = xc // nz, xm // nz, xf // nz
    cm, cf, ch = zm // LANES, zf // LANES, zh // LANES

    def buf(*shape):
        return pltpu.VMEM(shape, F32)

    def row(count, chunks, rows):
        return buf(count, chunks, rows, LANES)

    bm, bf = occ_m.shape[0] + 2, occ_f.shape[0] + 2
    scratch = [
        pltpu.VMEM(a.shape, a.dtype) for a in (rhs_c, rhs_m, rhs_f, occ_c, occ_m, occ_f)
    ]
    scratch += [pltpu.SMEM(args[6].shape, F32), pltpu.SemaphoreType.DMA((7,))]
    scratch += [
        buf(xc + 8, yc + 2 * TOP, zc), buf(xc + 8, yc + 2 * TOP, zc),
        buf(occ_c.shape[0] + 2, yc, zc),
        buf(2 * (xc + 6), ym + ROWS, zc), row(2 * (xc + 6), cm, ym + ROWS),
        buf(occ_c.shape[0] + 2, ROWS, LANES),
    ]
    scratch += [row(xm + 8, cm, ym + 2 * TOP)] * 8
    scratch += [
        row(bm, cm, ym + ROWS),
        buf(xm + 4, ym + ROWS, zm), buf(xm + 4, ym + ROWS, zf), row(xm + 4, cf, yf + ROWS),
        buf(bm, ROWS, LANES),
        row(xm + 6, cm, 4), row(xm + 6, cm, 4), row(xm + 6, cm, 4), row(xm + 6, cm, 4),
        buf(bm, ROWS, LANES), buf(bm, ROWS, LANES),
        row(xf + 8, cf, yf + 2 * TOP), row(bf, cf, yf + ROWS), buf(bf, ROWS, nz * LANES),
        row(xf + 2, ch, yf), row(3, ch, yf),
        row(xf + 3, cf, 1), row(xf + 3, cf, 2), row(xf + 3, cf, 1), row(xf + 3, cf, 2),
        buf(bf, ROWS, nz * LANES), buf(bf, ROWS, nz * LANES),
        buf(nx * ny * nz, 1, LANES), buf(nx * ny * nz, 1, LANES),
    ]
    for count in (64, nx * ny * nz, nx * ny * nz):
        scratch += [pltpu.SemaphoreType.DMA((count,))] * 2
    scratch += [pltpu.SemaphoreType.REGULAR((max(nx, ny),))]
    hbm = pl.BlockSpec(memory_space=pltpu.HBM)
    vmem = pl.BlockSpec(memory_space=pltpu.VMEM)
    field = pltpu.VMEM((xf + 8, cf, yf + 2 * TOP, LANES), F32)
    half = pltpu.VMEM((xf, ch, yf, LANES), F32)
    made_shapes = [pltpu.VMEM(a.shape, F32) for a in args[:2]]
    made_shapes += [field] * 3 + [half] * 3 + [pltpu.VMEM((2, ROWS, LANES), F32)]
    room = sum(4 * math.prod(a.shape) for a in made_shapes)
    made = pl.pallas_call(
        functools.partial(kernel, dims),
        out_shape=made_shapes,
        in_specs=[hbm] * 7,
        out_specs=[vmem] * 9,
        scratch_shapes=scratch,
        compiler_params=pltpu.CompilerParams(
            collective_id=0, has_side_effects=True, vmem_limit_bytes=VMEM_BYTES - room,
        ),
    )(*args)
    sol_c, sol_m, fields = made[0], made[1], made[2:]
    return pl.pallas_call(
        finish,
        out_shape=[jax.ShapeDtypeStruct(a.shape, F32) for a in args[:3]],
        in_specs=[vmem] * 9,
        out_specs=[hbm] * 3,
        scratch_shapes=[pltpu.VMEM(rhs_f.shape, F32), pltpu.SemaphoreType.DMA((6,))],
        compiler_params=pltpu.CompilerParams(vmem_limit_bytes=16 * 1024 * 1024),
    )(*fields, sol_c, sol_m)


def solution(mesh):
    dims = tuple(mesh.shape[axis] for axis in ("gx", "gy", "gz"))
    in_specs = (
        P("gx", None, None), P("gx", "gy", None), P("gx", "gy", "gz"),
        P("gx", None, None), P("gx", "gy", None), P("gx", "gy", "gz"), P(),
    )
    out_specs = (P("gx", None, None), P("gx", "gy", None), P("gx", "gy", "gz"))
    return jax.shard_map(
        functools.partial(shards, dims), mesh=mesh, in_specs=in_specs, out_specs=out_specs,
        check_vma=False,
    )
```

```python
import functools
import math

import jax
import jax.numpy as jnp
from jax import lax
from jax.experimental import pallas as pl
from jax.experimental.pallas import tpu as pltpu
from jax.sharding import PartitionSpec as P

MESH = pl.DeviceIdType.MESH
F32 = jnp.float32
BF16 = jnp.bfloat16
PAD = 4
ROWS = 8
TOP = 8
LANES = 128
VMEM_BYTES = 67043328


def iota(shape, dim):
    return lax.broadcasted_iota(jnp.int32, shape, dim)


def prolong_matrix(fine, coarse, total):
    base = lax.shift_right_arithmetic(fine, 1)
    beside = base + 2 * (fine & 1) - 1
    inside = jnp.logical_and(fine >= 0, fine < total)
    value = jnp.where(coarse == base, 0.75, jnp.where(coarse == beside, 0.25, 0.0))
    return jnp.where(inside, value, 0.0).astype(BF16)


def split(values):
    high = values.astype(BF16)
    return high, (values - high.astype(F32)).astype(BF16)


def mm(a, b):
    return jnp.dot(a, b, preferred_element_type=F32)


def fold_rows(values):
    total = values[0:ROWS]
    for row in range(ROWS, values.shape[0], ROWS):
        total = total + values[row : row + ROWS]
    out = total[:, 0:LANES]
    for lane in range(LANES, values.shape[1], LANES):
        out = out + total[:, lane : lane + LANES]
    return out


def coefficients(m0, n1, n2, n3):
    rho = n1 / m0
    spread = n2 - rho * n1
    bent = 6.0 * spread + (n3 - 2.0 * rho * n2 + rho * rho * n1)
    turn = jnp.where(bent > 0.0, jnp.maximum(spread, 0.0) / bent, 0.0)
    first = m0 / ((6.0 + rho) * m0 - jnp.maximum(spread, 0.0) * turn)
    second = -first * turn
    return first - second * rho, second


def kernel(
    dims,
    rhs_c, rhs_m, rhs_f, occ_c, occ_m, occ_f, weight_in,
    out_c, out_m, fg, fr, fw, tg, tr, tw, coef,
    in_c, in_m, in_f, io_c, io_m, io_f, weight, isem,
    cr, cw, cs, ctz, ct, oc,
    mb, g1, g2, u1, u2, v0, v1, v2, ms, mx, mtz, mt, om, m_up, m_dn, m_fu, m_fd, om_l, om_r,
    fb, fs, of, zsend, edge, f_up, f_dn, f_fu, f_fd, of_l, of_r,
    am, af, ss, rs, sm, rm, sf, rf, relay,
):
    nx, ny, nz = dims
    ix, iy, iz = lax.axis_index("gx"), lax.axis_index("gy"), lax.axis_index("gz")
    xc, yc, zc = rhs_c.shape
    xm, ym, zm = rhs_m.shape
    xf, yf, zh = rhs_f.shape
    zf = zh * nz
    xc, xm, xf = xc // nz, xm // nz, xf // nz
    cm, cf, ch = zm // LANES, zf // LANES, zh // LANES
    slab = ix * nz + iz
    slabs = nx * nz
    bc, bm, bf = occ_c.shape, occ_m.shape, occ_f.shape
    x_low, x_high = ix > 0, ix < nx - 1
    y_low, y_high = iy > 0, iy < ny - 1
    lower, upper = iz == 0, iz == 1
    first, last = slab == 0, slab == slabs - 1
    rows_c, rows_m, rows_f = (slice(TOP, TOP + n) for n in (yc, ym, yf))

    def both(a, b):
        return jnp.logical_and(a, b)

    def at(offset):
        return (
            lax.rem(ix + offset[0], nx), lax.rem(iy + offset[1], ny), lax.rem(iz + offset[2], nz)
        )

    loads = {}
    pairs = (
        ("c", rhs_c, in_c), ("oc", occ_c, io_c), ("om", occ_m, io_m), ("w", weight_in, weight),
        ("m", rhs_m, in_m), ("f", rhs_f, in_f), ("of", occ_f, io_f),
    )
    for k, (name, src, dst) in enumerate(pairs):
        loads[name] = pltpu.make_async_copy(src, dst, isem.at[k])
        loads[name].start()

    for ref in (oc, om, of, om_l, om_r, of_l, of_r):
        ref[...] = jnp.zeros_like(ref)

    barrier = pltpu.get_barrier_semaphore()
    peers = [(a, b, c) for a in range(nx) for b in range(ny) for c in range(nz)][1:]
    peers.sort(key=lambda o: (o[0] == 0) + (o[1] == 0))
    around = [(a, b) for a in (-1, 1, 0) for b in (-1, 1, 0)]

    def greet(semaphore, a, b, c):
        def send():
            pl.semaphore_signal(
                semaphore, inc=1, device_id=(ix + a, iy + b, c), device_id_type=MESH
            )

        tests = ((x_low, a < 0), (x_high, a > 0), (y_low, b < 0), (y_high, b > 0))
        there = [test for test, needed in tests if needed]
        if there:
            pl.when(functools.reduce(both, there))(send)
        else:
            send()

    for a, b in around:
        for c in range(1 if (a, b) == (0, 0) else 0, nz):
            greet(barrier, a, b, lax.rem(iz + c, nz))
    chips = (1 + jnp.where(x_low, 1, 0) + jnp.where(x_high, 1, 0)) * (
        1 + jnp.where(y_low, 1, 0) + jnp.where(y_high, 1, 0)
    )
    rounds = max(nx, ny) - 2

    def relay_send(k):
        if k < rounds:
            for a, b in around[:-1]:
                greet(relay.at[k], a, b, iz)

    def relay_wait(k):
        if k < rounds:
            pl.semaphore_wait(relay.at[k], chips - 1)

    def wipe(ref, planes):
        for p in planes:
            ref[p] = jnp.zeros(tuple(ref.shape[1:]), F32)

    @pl.when(first)
    def _():
        wipe(cr, range(0, 4))
        wipe(cs, (0,))
        wipe(mb, range(1, 4))
        wipe(fb, range(2, 4))
        for ref in (m_fu, m_fd):
            wipe(ref, range(0, 3))

    @pl.when(last)
    def _():
        wipe(cr, range(PAD + xc, PAD + xc + 4))
        wipe(cs, (bc[0] + 1,))
        wipe(mb, range(PAD + xm, PAD + xm + 3))
        wipe(fb, range(PAD + xf, PAD + xf + 2))
        for ref in (m_fu, m_fd):
            wipe(ref, range(xm + 3, xm + 6))

    @pl.when(jnp.logical_not(x_low))
    def _():
        for ref in (om_l, om_r, of_l, of_r):
            wipe(ref, (0,))

    @pl.when(jnp.logical_not(x_high))
    def _():
        for ref in (om_l, om_r, of_l, of_r):
            wipe(ref, (ref.shape[0] - 1,))

    @pl.when(jnp.logical_not(y_low))
    def _():
        for ref in (m_fu, f_fu, om_l, of_l):
            ref[...] = jnp.zeros_like(ref)

    @pl.when(jnp.logical_not(y_high))
    def _():
        for ref in (m_fd, f_fd, om_r, of_r):
            ref[...] = jnp.zeros_like(ref)

    loads["oc"].wait()
    oc[1 : 1 + bc[0], 0 : bc[1], 0 : bc[2]] = io_c[...].astype(F32)
    loads["om"].wait()
    om[1 : 1 + bm[0], 0 : bm[1], 0 : bm[2]] = io_m[...].astype(F32)
    loads["c"].wait()
    cr[pl.ds(PAD - 4 * iz, xc + 4), rows_c] = in_c[pl.ds(iz * (xc - 4), xc + 4)].astype(F32)

    def row_prolong(own, margin, index, total, cols, col_first):
        shape = (own + ROWS, cols)
        fine = iota(shape, 0) - margin + own * index
        return prolong_matrix(fine, iota(shape, 1) + col_first, total)

    def lane_prolong(cells, rows):
        shape = (rows, cells)
        return prolong_matrix(iota(shape, 1), iota(shape, 0), cells)

    def lane_bricks(cells, bricks, halves):
        shape = (halves * LANES, cells)
        brick = lax.div(iota(shape, 1), cells // (bricks * halves))
        place = brick + lax.div(brick, bricks) * (LANES - bricks)
        return (place == iota(shape, 0)).astype(BF16)

    def screens(put, begin, count, occ_parts, own, margin, bricks_y, lane_matrix, level):
        side = own // bricks_y
        cols = ROWS * len(occ_parts)
        shape = (own + 2 * margin if margin == 0 else own + ROWS, cols)
        brick = lax.div(iota(shape, 0) - margin + side, side) - 1
        place = jnp.where(
            brick < 0, ROWS + bricks_y - 1, jnp.where(brick >= bricks_y, 2 * ROWS, brick)
        )
        row_matrix = (place == iota(shape, 1)).astype(BF16)
        flags = [part[begin + x] for x in range(count) for part in occ_parts]
        wide = mm(jnp.concatenate(flags, axis=0).astype(BF16), lane_matrix).astype(BF16)
        for x in range(count):
            cells = mm(row_matrix, wide[x * cols : (x + 1) * cols])
            put(begin + x, weight[level] * (0.25 + cells))

    def chunked(ref):
        def put(j, value):
            for c in range(ref.shape[1]):
                ref[j, c] = value[:, c * LANES : (c + 1) * LANES]

        return put

    def put_coarse(j, value):
        cs[j] = value

    loads["w"].wait()
    screens(put_coarse, 1, bc[0], [oc], yc, 0, bc[1], lane_bricks(zc, bc[2], 1), 0)
    loads["m"].wait()
    held = pl.ds(3 - 3 * iz, xm + 3)
    for c in range(cm):
        cols = slice(c * LANES, (c + 1) * LANES)
        block = in_m[pl.ds(iz * (xm - 3), xm + 3), :, cols].astype(F32)
        mb[pl.ds(PAD - 3 * iz, xm + 3), c, rows_m] = block
        m_up[held, c] = block[:, ym - 4 : ym]
        m_dn[held, c] = block[:, 0:4]
    pl.semaphore_wait(barrier, chips * nz - 1)
    relay_send(0)

    used = [0]

    def copy(src, dst, target, step=0, count=1):
        k = used[0]
        used[0] += count

        def made(j):
            return pltpu.make_async_remote_copy(
                src_ref=src, dst_ref=dst, send_sem=ss.at[k], recv_sem=rs.at[k + j],
                device_id=target, device_id_type=MESH,
            )

        return made(0) if count == 1 else (made(step), [made(j) for j in range(count)])

    def start(items):
        for c, can_send, _ in items:
            if can_send is None:
                c.start()
            elif can_send is not False:
                pl.when(can_send)(c.start)

    def arrive(items):
        for c, _, can_recv in items:
            if can_recv is None:
                c.wait_recv()
            elif can_recv is not False:
                pl.when(can_recv)(c.wait_recv)

    def left(items):
        for c, can_send, _ in items:
            if can_send is None:
                c.wait_send()
            elif can_send is not False:
                pl.when(can_send)(c.wait_send)

    above, below = {"gx": ix + 1, "gz": 0}, {"gx": ix - 1, "gz": 1}
    send_up, get_low = both(upper, x_high), both(lower, x_low)
    send_down, get_high = both(lower, x_low), both(upper, x_high)

    def slab_swap(view, own, width_low, width_high, skip_low=0, skip_high=0):
        stop, begin = PAD + own - skip_low, PAD + skip_high
        low = PAD - skip_low - width_low
        return [
            (copy(view(stop - width_low, width_low), view(low, width_low), above),
             send_up, get_low),
            (copy(view(begin, width_high), view(begin + own, width_high), below),
             send_down, get_high),
        ]

    def brick_rows(bricks):
        return slice(0, bricks[1])

    def x_flags(occ, bricks, rows):
        return [
            (copy(occ.at[bricks, rows], occ.at[0, rows], {"gx": ix + 1}), x_high, x_low),
            (copy(occ.at[1, rows], occ.at[bricks + 1, rows], {"gx": ix - 1}), x_low, x_high),
        ]

    def y_flags(occ, occ_l, occ_r, bricks, rows):
        items = []
        flags = pl.ds(1, bricks)
        for dst, step, can_send, can_recv in (
            (occ_l, 1, y_high, y_low), (occ_r, -1, y_low, y_high)
        ):
            items.append((copy(occ.at[flags, rows], dst.at[flags, rows], {"gy": iy + step}), can_send, can_recv))
            items.append((copy(occ.at[bricks, rows], dst.at[0, rows], {"gx": ix + 1, "gy": iy + step}),
                          both(can_send, x_high), both(can_recv, x_low)))
            items.append((copy(occ.at[1, rows], dst.at[bricks + 1, rows], {"gx": ix - 1, "gy": iy + step}),
                          both(can_send, x_low), both(can_recv, x_high)))
        return items

    def coarse_view(begin, count):
        return cr.at[pl.ds(begin, count), rows_c]

    def mid_view(begin, count):
        return mb.at[pl.ds(begin, count), :, rows_m]

    near = slab_swap(coarse_view, xc, 1, 2)
    start(near)
    mid_flags = x_flags(om, bm[0], brick_rows(bm)) + y_flags(om, om_l, om_r, bm[0], brick_rows(bm))
    start(mid_flags)
    near_screens = [
        (copy(cs.at[bc[0]], cs.at[0], above), send_up, get_low),
        (copy(cs.at[1], cs.at[bc[0] + 1], below), send_down, get_high),
    ]
    start(near_screens)
    far = slab_swap(coarse_view, xc, 3, 2, 1, 2)
    start(far)

    mid_x = slab_swap(mid_view, xm, 3, 3)
    start(mid_x)
    mid_y = []
    for src, dst, step, can_send, can_recv in (
        (m_up, m_fu, 1, y_high, y_low), (m_dn, m_fd, -1, y_low, y_high)
    ):
        side = {"gy": iy + step}
        mid_y.append((copy(src.at[held], dst.at[held], side), can_send, can_recv))
        mid_y.append((copy(src.at[xm : xm + 3], dst.at[0:3], {**above, **side}),
                      both(can_send, send_up), both(can_recv, get_low)))
        mid_y.append((copy(src.at[3:6], dst.at[xm + 3 : xm + 6], {**below, **side}),
                      both(can_send, send_down), both(can_recv, get_high)))
    start(mid_y)

    loads["f"].wait()
    other = 1 - iz
    own_z, their_z = pl.ds(iz * ch, ch), pl.ds(other * ch, ch)

    def half_plane(p, c):
        return in_f[p, :, c * LANES : (c + 1) * LANES].astype(F32)

    def fill_fine(j, carry):
        for c in range(ch):
            zsend[j, c] = half_plane(other * (xf - 2) + j, c)
            fb[PAD - 2 * iz + j, iz * ch + c, rows_f] = half_plane(iz * (xf - 2) + j, c)
        return carry

    lax.fori_loop(0, xf + 2, fill_fine, 0, unroll=2)
    loads["of"].wait()
    own_flags = pl.ds(pl.multiple_of(iz * LANES, LANES), LANES)
    flags = jnp.concatenate(
        [io_f[...].astype(F32), jnp.zeros((bf[0], bf[1], LANES - bf[2]), F32)], axis=2
    )
    of[1 : 1 + bf[0], 0 : bf[1], own_flags] = flags
    partner = {"gz": other}
    z_fine = [
        (copy(zsend, fb.at[pl.ds(PAD - 2 * other, xf + 2), own_z, rows_f], partner), None, None),
        (copy(of.at[pl.ds(1, bf[0]), :, own_flags], of.at[pl.ds(1, bf[0]), :, own_flags], partner),
         None, None),
    ]
    start(z_fine[::-1])
    def wipe_rims(ref, own):
        shape = tuple(ref.shape)
        empty = jnp.zeros(shape[1:-2] + (TOP, LANES), F32)

        def one(p, carry):
            if len(shape) == 3:
                ref[p, 0:TOP] = empty
                ref[p, TOP + own :] = empty
            else:
                ref[p, :, 0:TOP] = empty
                ref[p, :, TOP + own :] = empty
            return carry

        lax.fori_loop(0, shape[0], one, 0)

    for ref in (cr, cw):
        wipe_rims(ref, yc)
    for ref in (mb, g1, g2, u1, u2, v0, v1, v2):
        wipe_rims(ref, ym)

    def z_lower(chunks):
        turned = [pltpu.roll(v, 1, 1) for v in chunks]
        edge_lane = iota(chunks[0].shape, 1) == 0
        return [
            jnp.where(edge_lane, turned[c - 1] if c else 0.0, turned[c])
            for c in range(len(chunks))
        ]

    def z_upper(chunks):
        turned = [pltpu.roll(v, LANES - 1, 1) for v in chunks]
        edge_lane = iota(chunks[0].shape, 1) == LANES - 1
        return [
            jnp.where(edge_lane, turned[c + 1] if c + 1 < len(chunks) else 0.0, turned[c])
            for c in range(len(chunks))
        ]

    def neighbours(load, chunks):
        low, high = z_lower(chunks), z_upper(chunks)
        return [
            (load(c, -1, 0) + load(c, 1, 0)) + (load(c, 0, -1) + load(c, 0, 1)) + (low[c] + high[c])
            for c in range(len(chunks))
        ]

    def later(load, chunks):
        high = z_upper(chunks)
        return [load(c, 1, 0) + load(c, 0, 1) + high[c] for c in range(len(chunks))]

    def view_of(ref, p, begin, count):
        def load(c, dx, dy):
            if len(ref.shape) == 3:
                return ref[p + dx, begin + dy : begin + dy + count]
            return ref[p + dx, c, begin + dy : begin + dy + count]

        return load, [load(c, 0, 0) for c in range(1 if len(ref.shape) == 3 else ref.shape[1])]

    def brick_of(own, side):
        return lambda p: lax.div(own * iz + p + (side - PAD), side)

    brick_c = brick_of(xc, nz * xc // bc[0])

    def coarse_w(p, carry):
        load, chunks = view_of(cr, p, TOP, yc)
        place = xc * slab + p - PAD
        keep = both(place >= 0, place < xc * slabs).astype(F32)
        cw[p, rows_c] = keep * (cs[brick_c(p)] * chunks[0] - neighbours(load, chunks)[0])
        return carry

    def coarse_moments(p, acc):
        load, chunks = view_of(cw, p, TOP, yc)
        r, w = cr[p, rows_c], chunks[0]
        image = cs[brick_c(p)] * w - 2.0 * later(load, chunks)[0]
        return tuple(a + fold_rows(b) for a, b in zip(acc, (r * r, r * w, w * w, w * image)))

    zero = jnp.zeros((ROWS, LANES), F32)
    lane_index = iota((1, LANES), 1)

    def spread_moments(values, buf, send, recv):
        row = jnp.zeros((1, LANES), F32)
        for k, a in values:
            value = jnp.sum(jnp.sum(a, axis=0, keepdims=True), axis=1, keepdims=True)
            row = jnp.where(lane_index == k, value, row)
        slot = (ix * ny + iy) * nz + iz
        buf[slot] = row
        copies = []
        for k, offset in enumerate(peers):
            c = pltpu.make_async_remote_copy(
                src_ref=buf.at[slot], dst_ref=buf.at[slot], send_sem=send.at[k],
                recv_sem=recv.at[k], device_id=at(offset), device_id_type=MESH,
            )
            c.start()
            copies.append(c)
        return copies

    def gathered(copies, buf):
        for c in copies:
            c.wait_recv()
        total = [buf[k] for k in range(buf.shape[0])]
        while len(total) > 1:
            total = [sum(total[k : k + 2][1:], total[k]) for k in range(0, len(total), 2)]
        return total[0]

    def picked(row, test):
        return jnp.sum(jnp.where(test, row, 0.0), axis=1, keepdims=True)

    def prolong(values, tz, put, lane_matrix, row_matrix):
        n, rows, lanes = values.shape
        high, low = split(values.reshape(n * rows, lanes))
        tz[...] = (mm(high, lane_matrix) + mm(low, lane_matrix)).reshape(tz.shape)
        twice = jnp.concatenate([row_matrix, row_matrix], axis=1)
        for j in range(n):
            put(j, mm(twice, jnp.concatenate(split(tz[j]), axis=0)))

    def interpolate(t, offset, count, g, own, begin, low, high, top):
        rows = t.shape[2]
        for p in range(PAD - low, PAD + own + high):
            m = p - PAD
            j = m // 2
            beside = min(max(j + (1 if m % 2 else -1) - begin, 0), count - 1)
            near_weight, side_weight = 0.75, 0.25
            if not 0 <= m < own:
                place = own * slab + m
                keep = both(place >= 0, place < own * slabs).astype(F32)
                near_weight, side_weight = 0.75 * keep, 0.25 * keep
            for c in range(t.shape[1]):
                g[p, c, top : top + rows] = (
                    near_weight * t[offset + j - begin, c] + side_weight * t[offset + beside, c]
                )

    def clear(ref, own, low, high):
        @pl.when(first)
        def _():
            wipe(ref, range(PAD - low, PAD))

        @pl.when(last)
        def _():
            wipe(ref, range(PAD + own, PAD + own + high))

    def row_masks(rows, margin, index, total):
        row = iota((rows + ROWS, LANES), 0) - margin + rows * index
        mask = both(row >= 0, row < total).astype(F32)
        return mask[0:ROWS], mask[rows:]

    def masked(v, masks):
        rows = v.shape[0] - ROWS
        return jnp.concatenate([v[0:ROWS] * masks[0], v[ROWS:rows], v[rows:] * masks[1]], axis=0)

    relay_wait(0)
    relay_send(1)
    for c in range(ch):
        for k, p in enumerate((0, 1, nz * xf - 1)):
            edge[k, c] = half_plane(p, c)
    pair_up, made_up = copy(
        edge.at[pl.ds(2, 1)], fb.at[pl.ds(PAD - 1, 1), own_z, rows_f], above, iz, nz
    )
    pair_dn, made_dn = copy(
        edge.at[pl.ds(0, 2)], fb.at[pl.ds(PAD + xf, 2), own_z, rows_f], below, iz, nz
    )
    fine_x = [(pair_up, x_high, False), (pair_dn, x_low, False)]
    fine_x += [(c, False, get_low) for c in made_up] + [(c, False, get_high) for c in made_dn]
    start(fine_x)

    arrive(near)
    arrive(near_screens)
    lax.fori_loop(PAD, PAD + xc + 1, coarse_w, 0, unroll=True)
    acc_c = lax.fori_loop(PAD, PAD + xc, coarse_moments, (zero,) * 4, unroll=True)
    mid_top = TOP - 4
    mid_lanes = lane_prolong(zm, zc)
    mid_rows = row_prolong(ym, 4, iy, ym * ny, yc, 0)
    arrive(z_fine)
    fine_flags = x_flags(of, bf[0], brick_rows(bf)) + y_flags(of, of_l, of_r, bf[0], brick_rows(bf))
    start(fine_flags)
    arrive(far)
    lax.fori_loop(1, PAD, coarse_w, 0, unroll=True)
    lax.fori_loop(PAD + xc + 1, PAD + xc + 3, coarse_w, 0, unroll=True)
    count_c = xc + 6
    twice_m = jnp.concatenate([mid_rows, mid_rows], axis=1)
    for j in range(count_c):
        planes = jnp.concatenate([cr[1 + j, rows_c], cw[1 + j, rows_c]], axis=1)
        made_rows = mm(twice_m, jnp.concatenate(split(planes), axis=0))
        ctz[j] = made_rows[:, 0:zc]
        ctz[count_c + j] = made_rows[:, zc:]
    high, low = split(ctz[...].reshape(2 * count_c * (ym + ROWS), zc))
    spread_z = mm(high, mid_lanes) + mm(low, mid_lanes)
    for c in range(cm):
        ct[:, c] = spread_z[:, c * LANES : (c + 1) * LANES].reshape(
            2 * count_c, ym + ROWS, LANES
        )
    for k, ref in enumerate((g1, g2)):
        interpolate(ct, k * count_c, count_c, ref, xm, -3, 4, 4, mid_top)
    arrive(mid_flags)
    screens(
        chunked(ms), 0, bm[0] + 2, [om, om_l, om_r], ym, 4, bm[1], lane_bricks(zm, bm[2], 1), 1
    )
    masks_m = row_masks(ym, 4, iy, ym * ny)
    brick_m = brick_of(xm, nz * xm // bm[0])
    window_m = slice(mid_top, mid_top + ym + ROWS)

    def mid_u(p, carry):
        brick = brick_m(p)
        for g, u in ((g1, u1), (g2, u2)):
            load, chunks = view_of(g, p, mid_top, ym + ROWS)
            for c, beside in enumerate(neighbours(load, chunks)):
                u[p, c, window_m] = masked((6.0 + ms[brick, c]) * chunks[c] - beside, masks_m)
        return carry

    lax.fori_loop(PAD - 3, PAD + xm + 3, mid_u, 0, unroll=True)
    for ref in (u1, u2):
        clear(ref, xm, 3, 3)
    arrive(mid_x)
    arrive(mid_y)
    for c in range(cm):
        mb[1 : xm + 7, c, TOP - 4 : TOP] = m_fu[:, c]
        mb[1 : xm + 7, c, TOP + ym : TOP + ym + 4] = m_fd[:, c]
    fields = ((mb, v0), (u1, v1), (u2, v2))

    def mid_v(p, carry):
        brick = brick_m(p)
        for u, v in fields:
            load, chunks = view_of(u, p, mid_top, ym + ROWS)
            for c, beside in enumerate(neighbours(load, chunks)):
                v[p, c, window_m] = masked(ms[brick, c] * chunks[c] - beside, masks_m)
        return carry

    lax.fori_loop(PAD - 2, PAD + xm + 2, mid_v, 0, unroll=True)
    for ref in (v0, v1, v2):
        clear(ref, xm, 2, 2)
    pairs_m = ((0, 0), (1, 1), (2, 2), (0, 1), (0, 2), (1, 2))

    def mid_moments(p, acc):
        brick = brick_m(p)
        views = [view_of(v, p, TOP, ym) for _, v in fields]
        beside = [later(load, chunks) for load, chunks in views]
        for c in range(cm):
            screen = ms[brick, c, 4 : 4 + ym]
            us = [u[p, c, rows_m] for u, _ in fields]
            vs = [chunks[c] for _, chunks in views]
            images = [screen * v - 2.0 * b[c] for v, b in zip(vs, beside)]
            values = [us[i] * us[j] for i, j in pairs_m] + [us[i] * vs[j] for i, j in pairs_m]
            values += [vs[i] * vs[j] for i, j in pairs_m]
            for i, j in pairs_m:
                cross = vs[i] * images[j]
                values.append(cross if i == j else 0.5 * (cross + vs[j] * images[i]))
            acc = tuple(a + fold_rows(v) for a, v in zip(acc, values))
        return acc

    acc = lax.fori_loop(PAD, PAD + xm, mid_moments, (zero,) * 24, unroll=2)
    relay_wait(1)
    for k in range(2, rounds):
        relay_send(k)
        relay_wait(k)
    slots = [(ROWS * (k // 6) + k % 6, a) for k, a in enumerate(acc)]
    slots += [(4 * ROWS + k, a) for k, a in enumerate(acc_c)]
    mid_copies = spread_moments(slots, am, sm, rm)

    arrive(fine_x)
    span = slice(PAD - 1, PAD + xf + 2)
    for c in range(cf):
        f_up[:, c] = fb[span, c, TOP + yf - 1 : TOP + yf]
        f_dn[:, c] = fb[span, c, TOP : TOP + 2]
    fine_y = [
        (copy(f_up, f_fu, {"gy": iy + 1}), y_high, y_low),
        (copy(f_dn, f_fd, {"gy": iy - 1}), y_low, y_high),
    ]
    start(fine_y)
    for ref in (fg, fr, fw):
        wipe_rims(ref, yf)
    fine_lanes = lane_prolong(zf, zm)
    fine_rows = row_prolong(yf, 2, iy, yf * ny, ym + ROWS, ym * iy - 4)
    masks_f = row_masks(yf, 2, iy, yf * ny)
    arrive(fine_flags)
    screens(
        chunked(fs), 0, bf[0] + 2, [of, of_l, of_r], yf, 2, bf[1], lane_bricks(zf, bf[2], nz), 2
    )
    arrive(fine_y)
    for c in range(cf):
        fb[span, c, TOP - 1 : TOP] = f_fu[:, c]
        fb[span, c, TOP + yf : TOP + yf + 2] = f_fd[:, c]
    total = gathered(mid_copies, am)
    ka, kb = coefficients(*[picked(total, lane_index == 4 * ROWS + k) for k in range(4)])
    weights = [None, ka * ka, kb * kb, -2.0 * ka, -2.0 * kb, 2.0 * ka * kb]
    kind = lane_index % ROWS
    scaled = total
    for k in range(1, 6):
        scaled = jnp.where(kind == k, total * weights[k], scaled)
    place = lax.div(lane_index, ROWS)
    km, kw = coefficients(*[
        picked(scaled, both(place == k, kind < 6)) for k in range(4)
    ])
    parts = (
        (g1, ka), (g2, kb), (mb, km), (u1, -km * ka), (u2, -km * kb),
        (v0, kw), (v1, -kw * ka), (v2, -kw * kb),
    )
    for p in range(2, xm + 6):
        for c in range(cm):
            value = parts[0][1] * parts[0][0][p, c, window_m]
            for ref, factor in parts[1:]:
                value = value + factor * ref[p, c, window_m]
            mx[p - 2, :, c * LANES : (c + 1) * LANES] = value
    own_c, own_m = pl.ds(iz * xc, xc), pl.ds(iz * xm, xm)

    prolong(mx[...], mtz, chunked(mt), fine_lanes, fine_rows)
    fine_top = TOP - 2
    interpolate(mt, 0, mt.shape[0], fg, xf, -2, 2, 3, fine_top)
    brick_f = brick_of(xf, nz * xf // bf[0])
    window_f = slice(fine_top, fine_top + yf + ROWS)

    def make_r(p, carry):
        brick = brick_f(p)
        load, chunks = view_of(fg, p, fine_top, yf + ROWS)
        for c, beside in enumerate(neighbours(load, chunks)):
            value = fb[p, c, window_f] - (6.0 + fs[brick, c]) * chunks[c] + beside
            fr[p, c, window_f] = masked(value, masks_f)
        return carry

    lax.fori_loop(PAD - 1, PAD + xf + 2, make_r, 0, unroll=True)
    clear(fr, xf, 1, 2)

    def make_w(p, carry):
        brick = brick_f(p)
        load, chunks = view_of(fr, p, fine_top, yf + ROWS)
        for c, beside in enumerate(neighbours(load, chunks)):
            fw[p, c, window_f] = masked(fs[brick, c] * chunks[c] - beside, masks_f)
        return carry

    lax.fori_loop(PAD, PAD + xf + 1, make_w, 0, unroll=True)
    clear(fw, xf, 0, 1)

    def moments(p, acc):
        brick = brick_f(p)
        load, chunks = view_of(fw, p, TOP, yf)
        for c, beside in enumerate(later(load, chunks)):
            r, w = fr[p, c, rows_f], chunks[c]
            image = fs[brick, c, 2 : 2 + yf] * w - 2.0 * beside
            acc = tuple(a + fold_rows(v) for a, v in zip(acc, (r * r, r * w, w * w, w * image)))
        return acc

    acc = lax.fori_loop(PAD, PAD + xf, moments, (zero,) * 4, unroll=True)
    fine_copies = spread_moments(list(enumerate(acc)), af, sf, rf)
    back = [
        (copy(src.at[PAD : PAD + xf, their_z, rows_f], dst, partner), None, None)
        for src, dst in ((fg, tg), (fr, tr), (fw, tw))
    ]
    start(back)
    out_c[own_c] = ka * cr[PAD : PAD + xc, rows_c] + kb * cw[PAD : PAD + xc, rows_c]
    out_m[own_m] = mx[2 : 2 + xm, 4 : 4 + ym, :]
    outs = [
        (copy(out_c.at[own_c], out_c.at[own_c], partner), None, None),
        (copy(out_m.at[own_m], out_m.at[own_m], partner), None, None),
    ]
    start(outs)
    for items in (
        near, near_screens, far, z_fine, mid_x, mid_flags, fine_x, mid_y, fine_flags, fine_y, outs
    ):
        left(items)
    for c in mid_copies:
        c.wait_send()
    arrive(outs)
    arrive(back)
    left(back)
    total = gathered(fine_copies, af)
    ka, kb = coefficients(*[picked(total, lane_index == k) for k in range(4)])
    coef[0] = jnp.broadcast_to(ka, (ROWS, LANES))
    coef[1] = jnp.broadcast_to(kb, (ROWS, LANES))
    for c in fine_copies:
        c.wait_send()


def finish(g, r, w, tg, tr, tw, coef, sol_c, sol_m, out_c, out_m, out_f, buf, sem):
    iz = lax.axis_index("gz")
    xs, ch, yf, _ = tg.shape
    small = [
        pltpu.make_async_copy(sol_c, out_c, sem.at[0]),
        pltpu.make_async_copy(sol_m, out_m, sem.at[1]),
    ]
    for c in small:
        c.start()
    ka, kb = coef[0, 0:1, 0:1], coef[1, 0:1, 0:1]
    rows = slice(TOP, TOP + yf)
    parts = 2
    step = xs // parts
    copies = list(small)
    for part in range(parts):
        for side in range(2):
            place = (iz if side == 0 else 1 - iz) * xs

            def one(x, carry):
                for c in range(ch):
                    if side == 0:
                        p, k = x + PAD, iz * ch + c
                        value = g[p, k, rows] + ka * r[p, k, rows] + kb * w[p, k, rows]
                    else:
                        value = tg[x, c] + ka * tr[x, c] + kb * tw[x, c]
                    buf[place + x, :, c * LANES : (c + 1) * LANES] = value
                return carry

            lax.fori_loop(part * step, part * step + step, one, 0, unroll=True)
            span = pl.ds(place + part * step, step)
            c = pltpu.make_async_copy(buf.at[span], out_f.at[span], sem.at[2 + 2 * part + side])
            c.start()
            copies.append(c)
    for c in copies:
        c.wait()


def shards(dims, *args):
    nx, ny, nz = dims
    rhs_c, rhs_m, rhs_f, occ_c, occ_m, occ_f, _ = args
    xc, yc, zc = rhs_c.shape
    xm, ym, zm = rhs_m.shape
    xf, yf, zh = rhs_f.shape
    zf = zh * nz
    xc, xm, xf = xc // nz, xm // nz, xf // nz
    cm, cf, ch = zm // LANES, zf // LANES, zh // LANES

    def buf(*shape):
        return pltpu.VMEM(shape, F32)

    def row(count, chunks, rows):
        return buf(count, chunks, rows, LANES)

    bm, bf = occ_m.shape[0] + 2, occ_f.shape[0] + 2
    scratch = [
        pltpu.VMEM(a.shape, a.dtype) for a in (rhs_c, rhs_m, rhs_f, occ_c, occ_m, occ_f)
    ]
    scratch += [pltpu.SMEM(args[6].shape, F32), pltpu.SemaphoreType.DMA((7,))]
    scratch += [
        buf(xc + 8, yc + 2 * TOP, zc), buf(xc + 8, yc + 2 * TOP, zc),
        buf(occ_c.shape[0] + 2, yc, zc),
        buf(2 * (xc + 6), ym + ROWS, zc), row(2 * (xc + 6), cm, ym + ROWS),
        buf(occ_c.shape[0] + 2, ROWS, LANES),
    ]
    scratch += [row(xm + 8, cm, ym + 2 * TOP)] * 8
    scratch += [
        row(bm, cm, ym + ROWS),
        buf(xm + 4, ym + ROWS, zm), buf(xm + 4, ym + ROWS, zf), row(xm + 4, cf, yf + ROWS),
        buf(bm, ROWS, LANES),
        row(xm + 6, cm, 4), row(xm + 6, cm, 4), row(xm + 6, cm, 4), row(xm + 6, cm, 4),
        buf(bm, ROWS, LANES), buf(bm, ROWS, LANES),
        row(xf + 8, cf, yf + 2 * TOP), row(bf, cf, yf + ROWS), buf(bf, ROWS, nz * LANES),
        row(xf + 2, ch, yf), row(3, ch, yf),
        row(xf + 3, cf, 1), row(xf + 3, cf, 2), row(xf + 3, cf, 1), row(xf + 3, cf, 2),
        buf(bf, ROWS, nz * LANES), buf(bf, ROWS, nz * LANES),
        buf(nx * ny * nz, 1, LANES), buf(nx * ny * nz, 1, LANES),
    ]
    for count in (64, nx * ny * nz, nx * ny * nz):
        scratch += [pltpu.SemaphoreType.DMA((count,))] * 2
    scratch += [pltpu.SemaphoreType.REGULAR((max(nx, ny),))]
    hbm = pl.BlockSpec(memory_space=pltpu.HBM)
    vmem = pl.BlockSpec(memory_space=pltpu.VMEM)
    field = pltpu.VMEM((xf + 8, cf, yf + 2 * TOP, LANES), F32)
    half = pltpu.VMEM((xf, ch, yf, LANES), F32)
    made_shapes = [pltpu.VMEM(a.shape, F32) for a in args[:2]]
    made_shapes += [field] * 3 + [half] * 3 + [pltpu.VMEM((2, ROWS, LANES), F32)]
    room = sum(4 * math.prod(a.shape) for a in made_shapes)
    made = pl.pallas_call(
        functools.partial(kernel, dims),
        out_shape=made_shapes,
        in_specs=[hbm] * 7,
        out_specs=[vmem] * 9,
        scratch_shapes=scratch,
        compiler_params=pltpu.CompilerParams(
            collective_id=0, has_side_effects=True, vmem_limit_bytes=VMEM_BYTES - room,
        ),
    )(*args)
    sol_c, sol_m, fields = made[0], made[1], made[2:]
    return pl.pallas_call(
        finish,
        out_shape=[jax.ShapeDtypeStruct(a.shape, F32) for a in args[:3]],
        in_specs=[vmem] * 9,
        out_specs=[hbm] * 3,
        scratch_shapes=[pltpu.VMEM(rhs_f.shape, F32), pltpu.SemaphoreType.DMA((6,))],
        compiler_params=pltpu.CompilerParams(vmem_limit_bytes=16 * 1024 * 1024),
    )(*fields, sol_c, sol_m)


def solution(mesh):
    dims = tuple(mesh.shape[axis] for axis in ("gx", "gy", "gz"))
    in_specs = (
        P("gx", None, None), P("gx", "gy", None), P("gx", "gy", "gz"),
        P("gx", None, None), P("gx", "gy", None), P("gx", "gy", "gz"), P(),
    )
    out_specs = (P("gx", None, None), P("gx", "gy", None), P("gx", "gy", "gz"))
    return jax.shard_map(
        functools.partial(shards, dims), mesh=mesh, in_specs=in_specs, out_specs=out_specs,
        check_vma=False,
    )
```
